256 devices in a mesh: span: 64 (over y, x, z_lo, core), head: 4 (over z_hi).
Axes of the slice: x: 4, y: 4, z: 8 (z_hi: 4, z_lo: 2; z = z_hi * 2 + z_lo), core: 2. Of those that a mesh axis runs over, the one named last changes fastest.
Arguments:
- decoder_states: bfloat16 [131072, 1024], P('span'), may hold values from -21 to 21
- encodings: bfloat16 [4096, 128, 1024], P('span', 'head'), may hold values from -21 to 21
- neighbor_table: int32 [2048, 2, 2], P('span'), may hold values from 0 to 63, as said below
- query_weight: bfloat16 [1024, 1024], P(None, 'head'), may hold values from -0.1875 to 0.1875
- key_weight: bfloat16 [1024, 1024], P(None, 'head'), may hold values from -0.1875 to 0.1875
- value_weight: bfloat16 [1024, 1024], P(None, 'head'), may hold values from -0.1875 to 0.1875
- out_weight: bfloat16 [1024, 1024], P('head'), may hold values from -0.1875 to 0.1875
Outputs:
- attended: bfloat16 [131072, 1024], P('span', 'head')
The draws below stay inside these ranges and needn't reach their ends.
Inputs may be any that keep to these rules, and one draw needn't show every extreme that they name: neighbor_table[c, k, 0] is the database shard and neighbor_table[c, k, 1] the slot in that shard of neighbor k of span c; in each aligned block of 32 spans (the spans of one device along `span`) every shard is named by exactly one neighbor, and every slot of every shard is named exactly once in the whole table.
All inputs are finite; a program needn't handle non-finite values.
Results may differ from the reference program's by a relative error of at most 0.012.
The reference program's roundings to bfloat16 on the way (of `keys`, `values`, `queries`, `weights` and `context`) count: a program that leaves them out, or rounds other values in their place, can miss the bound.
Values may be sent and summed in bfloat16 or wider, within the bound.
No kernel may reach another device: no remote copies, remote signals or barrier semaphores. Data moves between devices by JAX's collectives and lax.ppermute only.
A program may use at most 128 MiB of HBM per device.

```python
import jax
import jax.numpy as jnp
from jax import lax

D = 1024
HEADS = 16
HEAD_DIM = 64
SPAN_LEN = 64
NEIGH = 2
NTOK = 128
SEQ_LEN = 2048
SPANS_SEQ = 32
TOKENS = 131072
SPANS = 2048
SHARDS = 64
SLOTS = 64
PER_SOURCE = 1


def draw_decoder_states(key, part):
    subkeys = jax.random.split(jax.random.fold_in(key, 3), 1)
    values = jnp.clip(jax.random.normal(subkeys[0], (TOKENS, D), jnp.float32), -6.0, 6.0)
    return values.astype(jnp.bfloat16)


def draw_encodings(key, part):
    subkeys = jax.random.split(jax.random.fold_in(key, 5), 1)
    shape_all = (SHARDS * SLOTS, NTOK, D)
    values = jnp.clip(jax.random.normal(subkeys[0], shape_all, jnp.float32), -6.0, 6.0)
    return values.astype(jnp.bfloat16)


def draw_neighbor_table(key, part):
    dest_keys = jax.random.split(jax.random.fold_in(key, 11), SHARDS)
    orders = jax.vmap(lambda subkey: jax.random.permutation(subkey, SLOTS))(dest_keys).astype(jnp.int32)
    shard_of = orders // PER_SOURCE
    sub_index = orders % PER_SOURCE
    source_keys = jax.random.split(jax.random.fold_in(key, 12), SHARDS)
    slot_orders = jax.vmap(lambda subkey: jax.random.permutation(subkey, SLOTS))(source_keys).astype(jnp.int32)
    destination = jnp.arange(SHARDS, dtype=jnp.int32)[:, None]
    slot_of = slot_orders[shard_of, destination * PER_SOURCE + sub_index]
    return jnp.stack([shard_of, slot_of], axis=-1).reshape(SPANS, NEIGH, 2).astype(jnp.int32)


def steps_of(rng, dims, pieces, smallest, largest):
    def one(position, parts):
        draws = jax.random.uniform(jax.random.fold_in(jax.random.fold_in(rng, 6), position), (parts,), jnp.float32, smallest / len(pieces), largest / len(pieces))
        return jnp.repeat(jnp.exp(draws), dims[position] // parts).reshape((-1,) + (1,) * (len(dims) - position - 1))

    level = one(*pieces[0])
    for cut in pieces[1:]:
        level = level * one(*cut)
    return level


def normal_values(key, dims, spread, bound, pieces=(), kind=jnp.bfloat16):
    drawn = jax.random.normal(key, dims, jnp.float32) * spread
    if len(pieces) > 0:
        drawn = steps_of(key, dims, pieces, -0.22, 0.18) * drawn
    return jnp.clip(drawn, min=-bound, max=bound).astype(kind)


def setup_inputs(seed: int = 0) -> dict:
    keys = jax.random.split(jax.random.key(seed), 8)
    decoder_states = draw_decoder_states(jax.random.fold_in(keys[7], 71), 0)
    encodings = draw_encodings(jax.random.fold_in(keys[7], 71), 0)
    neighbor_table = draw_neighbor_table(jax.random.fold_in(keys[7], 71), 0)
    query_weight = normal_values(keys[3], (D, HEADS * HEAD_DIM), D ** -0.5, 0.1875, ((1, 4),))
    key_weight = normal_values(keys[4], (D, HEADS * HEAD_DIM), D ** -0.5, 0.1875, ((1, 4),))
    value_weight = normal_values(keys[5], (D, HEADS * HEAD_DIM), D ** -0.5, 0.1875, ((1, 4),))
    out_weight = normal_values(keys[6], (HEADS * HEAD_DIM, D), (HEADS * HEAD_DIM) ** -0.5, 0.1875, ((0, 4),))
    return dict(decoder_states=decoder_states, encodings=encodings, neighbor_table=neighbor_table, query_weight=query_weight, key_weight=key_weight, value_weight=value_weight, out_weight=out_weight)


def reference(decoder_states, encodings, neighbor_table, query_weight, key_weight, value_weight, out_weight):
    group_rows = (neighbor_table[:, :, 0] * SLOTS + neighbor_table[:, :, 1]).astype(jnp.int32)
    inv_root = HEAD_DIM ** -0.5
    offset = SPAN_LEN - 1
    inner_width = HEADS * HEAD_DIM

    def one_sequence(sequence):
        states = lax.dynamic_slice_in_dim(decoder_states, sequence * SEQ_LEN, SEQ_LEN, 0)
        chosen = lax.dynamic_slice_in_dim(group_rows, sequence * SPANS_SEQ, SPANS_SEQ, 0).reshape(-1)
        flattened = encodings[chosen].reshape(-1, D)
        key_rows = jnp.dot(flattened, key_weight, preferred_element_type=jnp.float32).astype(jnp.bfloat16)
        key_rows = key_rows.reshape(SPANS_SEQ, NEIGH * NTOK, HEADS, HEAD_DIM)
        value_rows = jnp.dot(flattened, value_weight, preferred_element_type=jnp.float32).astype(jnp.bfloat16)
        value_rows = value_rows.reshape(SPANS_SEQ, NEIGH * NTOK, HEADS, HEAD_DIM)
        queries = jnp.dot(states, query_weight, preferred_element_type=jnp.float32).astype(jnp.bfloat16)
        shifted = jnp.concatenate([queries[offset:], jnp.zeros((offset, inner_width), jnp.bfloat16)], axis=0)
        shifted = shifted.reshape(SPANS_SEQ, SPAN_LEN, HEADS, HEAD_DIM)
        scores = jnp.einsum("cqhd,ckhd->chqk", shifted.astype(jnp.float32), key_rows.astype(jnp.float32)) * inv_root
        weights = jax.nn.softmax(scores, axis=-1).astype(jnp.bfloat16)
        context = jnp.einsum("chqk,ckhd->cqhd", weights.astype(jnp.float32), value_rows.astype(jnp.float32))
        context = context.astype(jnp.bfloat16).reshape(SEQ_LEN, inner_width)
        context = jnp.concatenate([jnp.zeros((offset, inner_width), jnp.bfloat16), context[:SEQ_LEN - offset]], axis=0)
        return jnp.dot(context, out_weight, preferred_element_type=jnp.float32).astype(jnp.bfloat16)

    sequences = TOKENS // SEQ_LEN
    outputs = lax.map(one_sequence, jnp.arange(sequences, dtype=jnp.int32))
    return outputs.reshape(TOKENS, D)
```

```python
import functools

import jax
import jax.numpy as jnp
from jax import lax
from jax.experimental import pallas as pl
from jax.experimental.pallas import tpu as pltpu
from jax.sharding import PartitionSpec as P

HEAD_DIM = 64
SPAN_LEN = 64
SPANS_STEP = 2


def attention_kernel(head_ref, x_ref, now_ref, next_ref, w_ref, out_ref, k_ref, v_ref):
    f32, bf16 = jnp.float32, jnp.bfloat16
    parts, entries, piece, width = x_ref.shape
    spans = entries // 2
    keys = 2 * parts * piece
    groups = w_ref.shape[1]
    cols = width // groups
    rows = spans * SPAN_LEN

    x = jnp.concatenate(
        [x_ref[:, 2 * i : 2 * i + 2].reshape(keys, width) for i in range(spans)], axis=0
    )
    both = jnp.concatenate([now_ref[...], next_ref[...]], axis=0)
    row = lax.broadcasted_iota(jnp.int32, (rows, rows + SPAN_LEN), 0)
    col = lax.broadcasted_iota(jnp.int32, (rows, rows + SPAN_LEN), 1)
    shift = jnp.where(col == row + SPAN_LEN - 1, 1.0, 0.0).astype(bf16)
    states = jnp.dot(shift, both, preferred_element_type=f32).astype(bf16)

    def weight(which, g):
        return w_ref[:, g, :, which * cols : (which + 1) * cols].reshape(width, cols)

    total = jnp.zeros((rows, width), f32)
    lane = lax.broadcasted_iota(jnp.int32, (SPAN_LEN, 128), 1)
    low = lane < HEAD_DIM
    for g in range(groups):
        k_ref[...] = jnp.dot(x, weight(0, g), preferred_element_type=f32).astype(bf16)
        v_ref[...] = jnp.dot(x, weight(1, g), preferred_element_type=f32).astype(bf16)
        q = jnp.dot(states, weight(2, g), preferred_element_type=f32).astype(bf16)
        context_rows = []
        for i in range(spans):
            pieces = []
            for pair in range(cols // 128):
                here = slice(pair * 128, pair * 128 + 128)
                qp = q[i * SPAN_LEN : (i + 1) * SPAN_LEN, here]
                zero = jnp.zeros_like(qp)
                two = jnp.concatenate([jnp.where(low, qp, zero), jnp.where(low, zero, qp)], axis=0)
                kp = k_ref[i * keys : (i + 1) * keys, here]
                vp = v_ref[i * keys : (i + 1) * keys, here]
                scores = lax.dot_general(
                    two, kp, (((1,), (1,)), ((), ())), preferred_element_type=f32
                ) * (HEAD_DIM ** -0.5)
                top = jnp.max(scores, axis=1, keepdims=True)
                raised = jnp.exp(scores - top)
                weights = raised * (1.0 / jnp.sum(raised, axis=1, keepdims=True))
                mixed = jnp.dot(weights.astype(bf16), vp, preferred_element_type=f32)
                pieces.append(jnp.where(low, mixed[:SPAN_LEN], mixed[SPAN_LEN:]).astype(bf16))
            context_rows.append(jnp.concatenate(pieces, axis=1))
        context = jnp.concatenate(context_rows, axis=0)
        total = total + lax.dot_general(
            context, weight(3, g), (((1,), (1,)), ((), ())), preferred_element_type=f32
        )
    out_ref[...] = total.astype(bf16)


def attend(head, x, states, weights):
    parts, entries, piece, width = x.shape
    spans = entries // 2
    steps = spans // SPANS_STEP
    rows = SPANS_STEP * SPAN_LEN
    last = states.shape[0] // SPAN_LEN - 1
    keys = 2 * parts * piece
    cols = width // weights.shape[1]

    def after(i, head_ref):
        return jnp.minimum((head_ref[0] * steps + i + 1) * SPANS_STEP, last), 0

    flops = 2 * spans * (keys * width * 2 * width + SPAN_LEN * 2 * width * width)
    return pl.pallas_call(
        attention_kernel,
        out_shape=jax.ShapeDtypeStruct((spans * SPAN_LEN, width), jnp.bfloat16),
        grid_spec=pltpu.PrefetchScalarGridSpec(
            num_scalar_prefetch=1,
            grid=(steps,),
            in_specs=[
                pl.BlockSpec((parts, 2 * SPANS_STEP, piece, width), lambda i, h: (0, i, 0, 0)),
                pl.BlockSpec((rows, width), lambda i, h: (h[0] * steps + i, 0)),
                pl.BlockSpec((SPAN_LEN, width), after),
                pl.BlockSpec(memory_space=pltpu.VMEM),
            ],
            out_specs=pl.BlockSpec((rows, width), lambda i, h: (i, 0)),
            scratch_shapes=[
                pltpu.VMEM((SPANS_STEP * keys, cols), jnp.bfloat16),
                pltpu.VMEM((SPANS_STEP * keys, cols), jnp.bfloat16),
            ],
        ),
        compiler_params=pltpu.CompilerParams(
            dimension_semantics=("arbitrary",), vmem_limit_bytes=48 * 1024 * 1024
        ),
        cost_estimate=pl.CostEstimate(
            flops=flops, bytes_accessed=2 * (x.size + weights.size), transcendentals=0
        ),
        name="attend",
    )(head, x, states, states, weights)


def body(
    decoder_states, encodings, neighbor_table, query_weight, key_weight, value_weight, out_weight
):
    peers = lax.axis_size("span")
    groups = lax.axis_size("head")
    span = lax.axis_index("span")
    head = lax.axis_index("head")
    width = decoder_states.shape[1]

    depth = width // peers
    part = jnp.concatenate(
        [
            lax.dynamic_slice_in_dim(w, span * depth, depth, 0)
            for w in (key_weight, value_weight, query_weight)
        ]
        + [lax.dynamic_slice_in_dim(out_weight, span * depth, depth, 1).T],
        axis=1,
    )
    weights = lax.all_gather(part, ("span", "head"), axis=0, tiled=False)
    weights = weights.reshape(peers, groups, depth, width)

    shard_ids = neighbor_table[:, :, 0].reshape(-1)
    slot_ids = neighbor_table[:, :, 1].reshape(-1)
    entries = shard_ids.shape[0]
    numbering = jnp.arange(entries, dtype=jnp.int32)
    placed = shard_ids[None, :] == numbering[:, None]
    request = jnp.sum(jnp.where(placed, slot_ids[None, :], 0), axis=1)
    wanted = lax.all_to_all(request, "span", split_axis=0, concat_axis=0, tiled=True)
    arrived = lax.all_to_all(
        encodings[wanted], "span", split_axis=0, concat_axis=0, tiled=True
    )
    ordered = arrived[shard_ids]
    own = lax.all_to_all(
        ordered.reshape(groups, entries // groups, *arrived.shape[1:]),
        "head",
        split_axis=0,
        concat_axis=0,
        tiled=True,
    )
    result = attend(head.reshape(1), own, decoder_states, weights)
    columns = lax.all_to_all(result, "head", split_axis=1, concat_axis=0, tiled=True)
    offset = SPAN_LEN - 1
    return jnp.concatenate(
        [jnp.zeros((offset, columns.shape[1]), columns.dtype), columns[: columns.shape[0] - offset]],
        axis=0,
    )


def solution(mesh):
    return jax.shard_map(
        body,
        mesh=mesh,
        in_specs=(
            P("span", None),
            P("span", "head", None),
            P("span", None, None),
            P(None, "head"),
            P(None, "head"),
            P(None, "head"),
            P("head", None),
        ),
        out_specs=P("span", "head"),
        check_vma=False,
    )
```

```python
import functools

import jax
import jax.numpy as jnp
from jax import lax
from jax.experimental import pallas as pl
from jax.experimental.pallas import tpu as pltpu
from jax.sharding import PartitionSpec as P

HEAD_DIM = 64
SPAN_LEN = 64
SPANS_STEP = 2
SPAN = ("y", "x", "z", "core")


def attention_kernel(head_ref, x_ref, now_ref, next_ref, w_ref, out_ref, k_ref, v_ref):
    f32, bf16 = jnp.float32, jnp.bfloat16
    parts, entries, piece, width = x_ref.shape
    spans = entries // 2
    keys = 2 * parts * piece
    groups = w_ref.shape[1]
    cols = width // groups
    rows = spans * SPAN_LEN

    x = jnp.concatenate(
        [x_ref[:, 2 * i : 2 * i + 2].reshape(keys, width) for i in range(spans)], axis=0
    )
    both = jnp.concatenate([now_ref[...], next_ref[...]], axis=0)
    row = lax.broadcasted_iota(jnp.int32, (rows, rows + SPAN_LEN), 0)
    col = lax.broadcasted_iota(jnp.int32, (rows, rows + SPAN_LEN), 1)
    shift = jnp.where(col == row + SPAN_LEN - 1, 1.0, 0.0).astype(bf16)
    states = jnp.dot(shift, both, preferred_element_type=f32).astype(bf16)

    def weight(which, g):
        return w_ref[:, g, :, which * cols : (which + 1) * cols].reshape(width, cols)

    total = jnp.zeros((rows, width), f32)
    lane = lax.broadcasted_iota(jnp.int32, (SPAN_LEN, 128), 1)
    low = lane < HEAD_DIM
    for g in range(groups):
        k_ref[...] = jnp.dot(x, weight(0, g), preferred_element_type=f32).astype(bf16)
        v_ref[...] = jnp.dot(x, weight(1, g), preferred_element_type=f32).astype(bf16)
        q = jnp.dot(states, weight(2, g), preferred_element_type=f32).astype(bf16)
        context_rows = []
        for i in range(spans):
            pieces = []
            for pair in range(cols // 128):
                here = slice(pair * 128, pair * 128 + 128)
                qp = q[i * SPAN_LEN : (i + 1) * SPAN_LEN, here]
                zero = jnp.zeros_like(qp)
                two = jnp.concatenate([jnp.where(low, qp, zero), jnp.where(low, zero, qp)], axis=0)
                kp = k_ref[i * keys : (i + 1) * keys, here]
                vp = v_ref[i * keys : (i + 1) * keys, here]
                scores = lax.dot_general(
                    two, kp, (((1,), (1,)), ((), ())), preferred_element_type=f32
                ) * (HEAD_DIM ** -0.5)
                top = jnp.max(scores, axis=1, keepdims=True)
                raised = jnp.exp(scores - top)
                weights = raised * (1.0 / jnp.sum(raised, axis=1, keepdims=True))
                mixed = jnp.dot(weights.astype(bf16), vp, preferred_element_type=f32)
                pieces.append(jnp.where(low, mixed[:SPAN_LEN], mixed[SPAN_LEN:]).astype(bf16))
            context_rows.append(jnp.concatenate(pieces, axis=1))
        context = jnp.concatenate(context_rows, axis=0)
        total = total + lax.dot_general(
            context, weight(3, g), (((1,), (1,)), ((), ())), preferred_element_type=f32
        )
    out_ref[...] = total.astype(bf16)


def attend(head, x, states, weights):
    parts, entries, piece, width = x.shape
    spans = entries // 2
    steps = spans // SPANS_STEP
    rows = SPANS_STEP * SPAN_LEN
    last = states.shape[0] // SPAN_LEN - 1
    keys = 2 * parts * piece
    cols = width // weights.shape[1]

    def after(i, head_ref):
        return jnp.minimum((head_ref[0] * steps + i + 1) * SPANS_STEP, last), 0

    flops = 2 * spans * (keys * width * 2 * width + SPAN_LEN * 2 * width * width)
    return pl.pallas_call(
        attention_kernel,
        out_shape=jax.ShapeDtypeStruct((spans * SPAN_LEN, width), jnp.bfloat16),
        grid_spec=pltpu.PrefetchScalarGridSpec(
            num_scalar_prefetch=1,
            grid=(steps,),
            in_specs=[
                pl.BlockSpec((parts, 2 * SPANS_STEP, piece, width), lambda i, h: (0, i, 0, 0)),
                pl.BlockSpec((rows, width), lambda i, h: (h[0] * steps + i, 0)),
                pl.BlockSpec((SPAN_LEN, width), after),
                pl.BlockSpec(memory_space=pltpu.VMEM),
            ],
            out_specs=pl.BlockSpec((rows, width), lambda i, h: (i, 0)),
            scratch_shapes=[
                pltpu.VMEM((SPANS_STEP * keys, cols), jnp.bfloat16),
                pltpu.VMEM((SPANS_STEP * keys, cols), jnp.bfloat16),
            ],
        ),
        compiler_params=pltpu.CompilerParams(
            dimension_semantics=("arbitrary",), vmem_limit_bytes=48 * 1024 * 1024
        ),
        cost_estimate=pl.CostEstimate(
            flops=flops, bytes_accessed=2 * (x.size + weights.size), transcendentals=0
        ),
        name="attend",
    )(head, x, states, states, weights)


def body(
    decoder_states, encodings, neighbor_table, query_weight, key_weight, value_weight, out_weight
):
    peers = lax.axis_size(SPAN)
    groups = lax.axis_size("head")
    span = lax.axis_index(("core", "y", "z", "x"))
    head = lax.axis_index("head")
    width = decoder_states.shape[1]

    depth = width // peers
    part = jnp.concatenate(
        [
            lax.dynamic_slice_in_dim(w, span * depth, depth, 0)
            for w in (key_weight, value_weight, query_weight)
        ]
        + [lax.dynamic_slice_in_dim(out_weight, span * depth, depth, 1).T],
        axis=1,
    )
    near = ("x", "head")
    copies = jnp.broadcast_to(part[None], (lax.axis_size(near), depth, width))
    weights = lax.all_to_all(copies, near, split_axis=0, concat_axis=0, tiled=True)
    weights = lax.all_gather(weights, ("y", "z"), axis=0, tiled=True)
    weights = lax.all_gather(weights, "core", axis=0, tiled=True)
    weights = weights.reshape(peers, groups, depth, width)

    shard_ids = neighbor_table[:, :, 0].reshape(-1)
    slot_ids = neighbor_table[:, :, 1].reshape(-1)
    entries = shard_ids.shape[0]
    numbering = jnp.arange(entries, dtype=jnp.int32)
    placed = shard_ids[None, :] == numbering[:, None]
    request = jnp.sum(jnp.where(placed, slot_ids[None, :], 0), axis=1)
    wanted = lax.all_to_all(request, SPAN, split_axis=0, concat_axis=0, tiled=True)
    arrived = lax.all_to_all(
        encodings[wanted], SPAN, split_axis=0, concat_axis=0, tiled=True
    )
    ordered = arrived[shard_ids]
    own = lax.all_to_all(
        ordered.reshape(groups, entries // groups, *arrived.shape[1:]),
        "head",
        split_axis=0,
        concat_axis=0,
        tiled=True,
    )
    result = attend(head.reshape(1), own, decoder_states, weights)
    columns = lax.all_to_all(result, "head", split_axis=1, concat_axis=0, tiled=True)
    offset = SPAN_LEN - 1
    return jnp.concatenate(
        [jnp.zeros((offset, columns.shape[1]), columns.dtype), columns[: columns.shape[0] - offset]],
        axis=0,
    )


def solution(mesh):
    fine = jax.sharding.Mesh(mesh.devices.reshape(4, 4, 2, 2, 4), SPAN + ("head",))
    return jax.shard_map(
        body,
        mesh=fine,
        in_specs=(
            P(SPAN, None),
            P(SPAN, "head", None),
            P(SPAN, None, None),
            P(None, "head"),
            P(None, "head"),
            P(None, "head"),
            P("head", None),
        ),
        out_specs=P(SPAN, "head"),
        check_vma=False,
    )
```

```python
import jax
import jax.numpy as jnp
from jax import lax
from jax.experimental import pallas as pl
from jax.experimental.pallas import tpu as pltpu
from jax.sharding import PartitionSpec as P


HEAD_DIM = 64
SPAN_LEN = 64
SPANS_STEP = 2
CHUNKS = 2
SPAN = ("y", "x", "z", "core")


def attention_kernel(where_ref, *refs):
    x_refs = refs[:-8]
    now_ref, next_ref, own_ref, other_ref, out_ref, k_ref, v_ref, w_ref = refs[-8:]
    f32, bf16 = jnp.float32, jnp.bfloat16
    entries, piece, width = x_refs[0].shape
    spans = entries // 2
    some = 2 * piece
    keys = len(x_refs) * some
    groups = own_ref.shape[1]
    cols = width // groups

    @pl.when(pl.program_id(0) == 0)
    def _():
        core = where_ref[1]
        w_ref[core] = own_ref[...]
        w_ref[1 - core] = other_ref[...]

    rows = spans * SPAN_LEN

    x = jnp.concatenate(
        [
            x_ref[2 * i : 2 * i + 2].reshape(some, width)
            for i in range(spans)
            for x_ref in x_refs
        ],
        axis=0,
    )
    both = jnp.concatenate([now_ref[...], next_ref[...]], axis=0)
    row = lax.broadcasted_iota(jnp.int32, (rows, rows + SPAN_LEN), 0)
    col = lax.broadcasted_iota(jnp.int32, (rows, rows + SPAN_LEN), 1)
    shift = jnp.where(col == row + SPAN_LEN - 1, 1.0, 0.0).astype(bf16)
    states = jnp.dot(shift, both, preferred_element_type=f32).astype(bf16)

    def weight(which, g):
        return w_ref[:, :, g, :, which * cols : (which + 1) * cols].reshape(width, cols)

    total = jnp.zeros((rows, width), f32)
    lane = lax.broadcasted_iota(jnp.int32, (SPAN_LEN, 128), 1)
    low = lane < HEAD_DIM
    for g in range(groups):
        k_ref[...] = jnp.dot(x, weight(0, g), preferred_element_type=f32).astype(bf16)
        v_ref[...] = jnp.dot(x, weight(1, g), preferred_element_type=f32).astype(bf16)
        q = jnp.dot(states, weight(2, g), preferred_element_type=f32).astype(bf16)
        context_rows = []
        for i in range(spans):
            pieces = []
            for pair in range(cols // 128):
                here = slice(pair * 128, pair * 128 + 128)
                qp = q[i * SPAN_LEN : (i + 1) * SPAN_LEN, here]
                zero = jnp.zeros_like(qp)
                two = jnp.concatenate([jnp.where(low, qp, zero), jnp.where(low, zero, qp)], axis=0)
                kp = k_ref[i * keys : (i + 1) * keys, here]
                vp = v_ref[i * keys : (i + 1) * keys, here]
                scores = lax.dot_general(
                    two, kp, (((1,), (1,)), ((), ())), preferred_element_type=f32
                ) * (HEAD_DIM ** -0.5)
                top = jnp.max(scores, axis=1, keepdims=True)
                raised = jnp.exp(scores - top)
                weights = raised * (1.0 / jnp.sum(raised, axis=1, keepdims=True))
                mixed = jnp.dot(weights.astype(bf16), vp, preferred_element_type=f32)
                pieces.append(jnp.where(low, mixed[:SPAN_LEN], mixed[SPAN_LEN:]).astype(bf16))
            context_rows.append(jnp.concatenate(pieces, axis=1))
        context = jnp.concatenate(context_rows, axis=0)
        total = total + lax.dot_general(
            context, weight(3, g), (((1,), (1,)), ((), ())), preferred_element_type=f32
        )
    for g in range(groups):
        out_ref[g] = total[:, g * cols : (g + 1) * cols].astype(bf16)


def attend(where, chunks, states, weights, other):
    entries, piece, width = chunks[0].shape
    spans = entries // 2
    steps = spans // SPANS_STEP
    rows = SPANS_STEP * SPAN_LEN
    last = states.shape[0] // SPAN_LEN - 1
    keys = 2 * piece * len(chunks)
    groups = weights.shape[1]
    cols = width // groups

    def after(i, where_ref):
        return jnp.minimum((where_ref[0] * steps + i + 1) * SPANS_STEP, last), 0

    flops = 2 * spans * (keys * width * 2 * width + SPAN_LEN * 2 * width * width)
    return pl.pallas_call(
        attention_kernel,
        out_shape=jax.ShapeDtypeStruct((groups, spans * SPAN_LEN, cols), jnp.bfloat16),
        grid_spec=pltpu.PrefetchScalarGridSpec(
            num_scalar_prefetch=1,
            grid=(steps,),
            in_specs=[
                pl.BlockSpec((2 * SPANS_STEP, piece, width), lambda i, h: (i, 0, 0))
                for _ in chunks
            ]
            + [
                pl.BlockSpec((rows, width), lambda i, h: (h[0] * steps + i, 0)),
                pl.BlockSpec((SPAN_LEN, width), after),
                pl.BlockSpec(memory_space=pltpu.VMEM),
                pl.BlockSpec(memory_space=pltpu.VMEM),
            ],
            out_specs=pl.BlockSpec((groups, rows, cols), lambda i, h: (0, i, 0)),
            scratch_shapes=[
                pltpu.VMEM((SPANS_STEP * keys, cols), jnp.bfloat16),
                pltpu.VMEM((SPANS_STEP * keys, cols), jnp.bfloat16),
                pltpu.VMEM((2, *weights.shape), jnp.bfloat16),
            ],
        ),
        compiler_params=pltpu.CompilerParams(
            dimension_semantics=("arbitrary",), vmem_limit_bytes=48 * 1024 * 1024
        ),
        cost_estimate=pl.CostEstimate(
            flops=flops, bytes_accessed=2 * (len(chunks) * chunks[0].size + 2 * weights.size), transcendentals=0
        ),
        name="attend",
    )(where, *chunks, states, states, weights, other)


def layer(
    decoder_states, encodings, neighbor_table, query_weight, key_weight, value_weight, out_weight
):
    peers = lax.axis_size(SPAN)
    groups = lax.axis_size("head")
    span = lax.axis_index(("core", "y", "x", "z"))
    head = lax.axis_index("head")
    width = decoder_states.shape[1]

    depth = width // peers
    part = jnp.concatenate(
        [
            lax.dynamic_slice_in_dim(w, span * depth, depth, 0)
            for w in (key_weight, value_weight, query_weight)
        ]
        + [lax.dynamic_slice_in_dim(out_weight, span * depth, depth, 1).T],
        axis=1,
    )
    column = ("z", "head")
    planes = lax.axis_size(column)
    place = lax.axis_index(column)
    passed = [part] + [
        lax.ppermute(part, column, [(i, (i + step) % planes) for i in range(planes)])
        for step in range(1, planes)
    ]
    order = (place - jnp.arange(planes, dtype=jnp.int32)) % planes
    stacked = jnp.stack(passed)[order]
    shard_ids = neighbor_table[:, :, 0].reshape(-1)
    slot_ids = neighbor_table[:, :, 1].reshape(-1)
    entries = shard_ids.shape[0]
    numbering = jnp.arange(entries, dtype=jnp.int32)
    placed = shard_ids[None, :] == numbering[:, None]
    request = jnp.sum(jnp.where(placed, slot_ids[None, :], 0), axis=1)
    wanted = lax.all_to_all(request, SPAN, split_axis=0, concat_axis=0, tiled=True)
    stacked, wanted = lax.optimization_barrier((stacked, wanted))
    weights = lax.all_gather(stacked, ("y", "x"), axis=0, tiled=True)
    piece = encodings.shape[1] // CHUNKS
    pieces = encodings.reshape(-1, piece, width)
    sources = shard_ids.reshape(groups, -1)
    owned = []
    for c in range(CHUNKS):
        arrived = lax.all_to_all(
            pieces[CHUNKS * wanted + c], SPAN, split_axis=0, concat_axis=0, tiled=True
        )
        for step in range(groups):
            block = arrived[sources[(head + step) % groups]]
            if step:
                block = lax.ppermute(
                    block, "head", [(i, (i + step) % groups) for i in range(groups)]
                )
            owned.append(block)
    weights = weights.reshape(peers // 2, groups, depth, width)
    other = lax.ppermute(weights, "core", [(0, 1), (1, 0)])
    where = jnp.stack([head, lax.axis_index("core")])
    result = attend(where, owned, decoder_states, weights, other)
    columns = lax.all_to_all(result, "head", split_axis=0, concat_axis=0, tiled=True)
    columns = columns.reshape(decoder_states.shape[0], width // groups)
    offset = SPAN_LEN - 1
    return jnp.concatenate(
        [jnp.zeros((offset, columns.shape[1]), columns.dtype), columns[: columns.shape[0] - offset]],
        axis=0,
    )


def solution(mesh):
    fine = jax.sharding.Mesh(mesh.devices.reshape(4, 4, 2, 2, 4), SPAN + ("head",))
    return jax.shard_map(
        layer,
        mesh=fine,
        in_specs=(
            P(SPAN, None),
            P(SPAN, "head", None),
            P(SPAN, None, None),
            P(None, "head"),
            P(None, "head"),
            P(None, "head"),
            P("head", None),
        ),
        out_specs=P(SPAN, "head"),
        check_vma=False,
    )
```

```python
import jax
import jax.numpy as jnp
from jax import lax
from jax.experimental import pallas as pl
from jax.experimental.pallas import tpu as pltpu
from jax.sharding import PartitionSpec as P


HEAD_DIM = 64
SPAN_LEN = 64
SPANS_STEP = 2
CHUNKS = 2
SPAN = ("y", "x", "z", "core")


def attention_kernel(where_ref, *refs):
    x_refs = refs[:-8]
    now_ref, next_ref, own_ref, other_ref, out_ref, k_ref, v_ref, w_ref = refs[-8:]
    f32, bf16 = jnp.float32, jnp.bfloat16
    entries, piece, width = x_refs[0].shape
    spans = entries // 2
    some = 2 * piece
    keys = len(x_refs) * some
    groups = own_ref.shape[1]
    cols = width // groups

    @pl.when(pl.program_id(0) == 0)
    def _():
        core = where_ref[1]
        w_ref[core] = own_ref[...]
        w_ref[1 - core] = other_ref[...]

    rows = spans * SPAN_LEN

    x = jnp.concatenate(
        [
            x_ref[2 * i : 2 * i + 2].reshape(some, width)
            for i in range(spans)
            for x_ref in x_refs
        ],
        axis=0,
    )
    both = jnp.concatenate([now_ref[...], next_ref[...]], axis=0)
    row = lax.broadcasted_iota(jnp.int32, (rows, rows + SPAN_LEN), 0)
    col = lax.broadcasted_iota(jnp.int32, (rows, rows + SPAN_LEN), 1)
    shift = jnp.where(col == row + SPAN_LEN - 1, 1.0, 0.0).astype(bf16)
    states = jnp.dot(shift, both, preferred_element_type=f32).astype(bf16)

    def weight(which, g):
        return w_ref[:, :, g, :, which * cols : (which + 1) * cols].reshape(width, cols)

    total = jnp.zeros((rows, width), f32)
    lane = lax.broadcasted_iota(jnp.int32, (SPAN_LEN, 128), 1)
    low = lane < HEAD_DIM
    for g in range(groups):
        k_ref[...] = jnp.dot(x, weight(0, g), preferred_element_type=f32).astype(bf16)
        v_ref[...] = jnp.dot(x, weight(1, g), preferred_element_type=f32).astype(bf16)
        q = jnp.dot(states, weight(2, g), preferred_element_type=f32).astype(bf16)
        context_rows = []
        for i in range(spans):
            pieces = []
            for pair in range(cols // 128):
                here = slice(pair * 128, pair * 128 + 128)
                qp = q[i * SPAN_LEN : (i + 1) * SPAN_LEN, here]
                zero = jnp.zeros_like(qp)
                two = jnp.concatenate([jnp.where(low, qp, zero), jnp.where(low, zero, qp)], axis=0)
                kp = k_ref[i * keys : (i + 1) * keys, here]
                vp = v_ref[i * keys : (i + 1) * keys, here]
                scores = lax.dot_general(
                    two, kp, (((1,), (1,)), ((), ())), preferred_element_type=f32
                ) * (HEAD_DIM ** -0.5)
                top = jnp.max(scores, axis=1, keepdims=True)
                raised = jnp.exp(scores - top)
                weights = raised * (1.0 / jnp.sum(raised, axis=1, keepdims=True))
                mixed = jnp.dot(weights.astype(bf16), vp, preferred_element_type=f32)
                pieces.append(jnp.where(low, mixed[:SPAN_LEN], mixed[SPAN_LEN:]).astype(bf16))
            context_rows.append(jnp.concatenate(pieces, axis=1))
        context = jnp.concatenate(context_rows, axis=0)
        total = total + lax.dot_general(
            context, weight(3, g), (((1,), (1,)), ((), ())), preferred_element_type=f32
        )
    for g in range(groups):
        out_ref[g] = total[:, g * cols : (g + 1) * cols].astype(bf16)


def attend(where, chunks, states, weights, other):
    entries, piece, width = chunks[0].shape
    spans = entries // 2
    steps = spans // SPANS_STEP
    rows = SPANS_STEP * SPAN_LEN
    last = states.shape[0] // SPAN_LEN - 1
    keys = 2 * piece * len(chunks)
    groups = weights.shape[1]
    cols = width // groups

    def after(i, where_ref):
        return jnp.minimum((where_ref[0] * steps + i + 1) * SPANS_STEP, last), 0

    flops = 2 * spans * (keys * width * 2 * width + SPAN_LEN * 2 * width * width)
    return pl.pallas_call(
        attention_kernel,
        out_shape=jax.ShapeDtypeStruct((groups, spans * SPAN_LEN, cols), jnp.bfloat16),
        grid_spec=pltpu.PrefetchScalarGridSpec(
            num_scalar_prefetch=1,
            grid=(steps,),
            in_specs=[
                pl.BlockSpec((2 * SPANS_STEP, piece, width), lambda i, h: (i, 0, 0))
                for _ in chunks
            ]
            + [
                pl.BlockSpec((rows, width), lambda i, h: (h[0] * steps + i, 0)),
                pl.BlockSpec((SPAN_LEN, width), after),
                pl.BlockSpec(memory_space=pltpu.VMEM),
                pl.BlockSpec(memory_space=pltpu.VMEM),
            ],
            out_specs=pl.BlockSpec((groups, rows, cols), lambda i, h: (0, i, 0)),
            scratch_shapes=[
                pltpu.VMEM((SPANS_STEP * keys, cols), jnp.bfloat16),
                pltpu.VMEM((SPANS_STEP * keys, cols), jnp.bfloat16),
                pltpu.VMEM((2, *weights.shape), jnp.bfloat16),
            ],
        ),
        compiler_params=pltpu.CompilerParams(
            dimension_semantics=("arbitrary",), vmem_limit_bytes=48 * 1024 * 1024
        ),
        cost_estimate=pl.CostEstimate(
            flops=flops, bytes_accessed=2 * (len(chunks) * chunks[0].size + 2 * weights.size), transcendentals=0
        ),
        name="attend",
    )(where, *chunks, states, states, weights, other)


def span_groups(peers, groups, turn):
    low = [(s // 2) % 2 == 0 for s in range(peers)]
    return [
        [s * groups + (h + (turn if low[s] else 0)) % groups for s in range(peers)]
        for h in range(groups)
    ]


def layer(
    decoder_states, encodings, neighbor_table, query_weight, key_weight, value_weight, out_weight
):
    peers = lax.axis_size(SPAN)
    groups = lax.axis_size("head")
    span = lax.axis_index(("core", "y", "x", "z"))
    head = lax.axis_index("head")
    width = decoder_states.shape[1]

    depth = width // peers
    part = jnp.concatenate(
        [
            lax.dynamic_slice_in_dim(w, span * depth, depth, 0)
            for w in (key_weight, value_weight, query_weight)
        ]
        + [lax.dynamic_slice_in_dim(out_weight, span * depth, depth, 1).T],
        axis=1,
    )
    column = ("z", "head")
    planes = lax.axis_size(column)
    place = lax.axis_index(column)
    passed = [part]
    for step in range(1, planes):
        passed.append(lax.ppermute(part, column, [(i, (i + step) % planes) for i in range(planes)]))
    order = (place - jnp.arange(planes, dtype=jnp.int32)) % planes
    stacked = jnp.stack(passed)[order]
    shard_ids = neighbor_table[:, :, 0].reshape(-1)
    slot_ids = neighbor_table[:, :, 1].reshape(-1)
    entries = shard_ids.shape[0]
    numbering = jnp.arange(entries, dtype=jnp.int32)
    placed = shard_ids[None, :] == numbering[:, None]
    request = jnp.sum(jnp.where(placed, slot_ids[None, :], 0), axis=1)
    wanted = lax.all_to_all(request, SPAN, split_axis=0, concat_axis=0, tiled=True)
    weights = lax.all_gather(stacked, ("y", "x"), axis=0, tiled=True)
    piece = encodings.shape[1] // CHUNKS
    pieces = encodings.reshape(-1, piece, width)
    sources = shard_ids.reshape(groups, -1)
    owned = []
    for c in range(CHUNKS):
        arrived = lax.all_to_all(
            pieces[CHUNKS * wanted + c],
            SPAN + ("head",),
            split_axis=0,
            concat_axis=0,
            axis_index_groups=span_groups(peers, groups, c % 2),
            tiled=True,
        )
        for step in range(groups):
            block = arrived[sources[(head + step) % groups]]
            if step:
                block = lax.ppermute(
                    block, "head", [(i, (i + step) % groups) for i in range(groups)]
                )
            owned.append(block)
    weights = weights.reshape(peers // 2, groups, depth, width)
    other = lax.ppermute(weights, "core", [(0, 1), (1, 0)])
    where = jnp.stack([head, lax.axis_index("core")])
    result = attend(where, owned, decoder_states, weights, other)
    columns = lax.all_to_all(result, "head", split_axis=0, concat_axis=0, tiled=True)
    columns = columns.reshape(decoder_states.shape[0], width // groups)
    offset = SPAN_LEN - 1
    return jnp.concatenate(
        [jnp.zeros((offset, columns.shape[1]), columns.dtype), columns[: columns.shape[0] - offset]],
        axis=0,
    )


def solution(mesh):
    fine = jax.sharding.Mesh(mesh.devices.reshape(4, 4, 2, 2, 4), SPAN + ("head",))
    return jax.shard_map(
        layer,
        mesh=fine,
        in_specs=(
            P(SPAN, None),
            P(SPAN, "head", None),
            P(SPAN, None, None),
            P(None, "head"),
            P(None, "head"),
            P(None, "head"),
            P("head", None),
        ),
        out_specs=P(SPAN, "head"),
        check_vma=False,
    )
```

```python
import jax
import jax.numpy as jnp
from jax import lax
from jax.experimental import pallas as pl
from jax.experimental.pallas import tpu as pltpu
from jax.sharding import PartitionSpec as P


HEAD_DIM = 64
SPAN_LEN = 64
SPANS_STEP = 2
CHUNKS = 4
SPAN = ("y", "x", "z", "core")


def attention_kernel(where_ref, *refs):
    x_refs = refs[:-8]
    now_ref, next_ref, own_ref, other_ref, out_ref, k_ref, v_ref, w_ref = refs[-8:]
    f32, bf16 = jnp.float32, jnp.bfloat16
    spans = SPANS_STEP
    some, width = x_refs[0].shape
    some //= spans
    keys = len(x_refs) * some
    groups = own_ref.shape[1]
    cols = width // groups

    @pl.when(pl.program_id(0) == 0)
    def _():
        core = where_ref[1]
        w_ref[core] = own_ref[...]
        w_ref[1 - core] = other_ref[...]

    rows = spans * SPAN_LEN

    x = jnp.concatenate(
        [
            x_ref[i * some : (i + 1) * some]
            for i in range(spans)
            for x_ref in x_refs
        ],
        axis=0,
    )
    both = jnp.concatenate([now_ref[...], next_ref[...]], axis=0)
    row = lax.broadcasted_iota(jnp.int32, (rows, rows + SPAN_LEN), 0)
    col = lax.broadcasted_iota(jnp.int32, (rows, rows + SPAN_LEN), 1)
    shift = jnp.where(col == row + SPAN_LEN - 1, 1.0, 0.0).astype(bf16)
    states = jnp.dot(shift, both, preferred_element_type=f32).astype(bf16)

    def weight(which, g):
        return w_ref[:, :, g, :, which * cols : (which + 1) * cols].reshape(width, cols)

    total = jnp.zeros((rows, width), f32)
    lane = lax.broadcasted_iota(jnp.int32, (SPAN_LEN, 128), 1)
    low = lane < HEAD_DIM
    for g in range(groups):
        k_ref[...] = jnp.dot(x, weight(0, g), preferred_element_type=f32).astype(bf16)
        v_ref[...] = jnp.dot(x, weight(1, g), preferred_element_type=f32).astype(bf16)
        q = jnp.dot(states, weight(2, g), preferred_element_type=f32).astype(bf16)
        context_rows = []
        for i in range(spans):
            pieces = []
            for pair in range(cols // 128):
                here = slice(pair * 128, pair * 128 + 128)
                qp = q[i * SPAN_LEN : (i + 1) * SPAN_LEN, here]
                zero = jnp.zeros_like(qp)
                two = jnp.concatenate([jnp.where(low, qp, zero), jnp.where(low, zero, qp)], axis=0)
                kp = k_ref[i * keys : (i + 1) * keys, here]
                vp = v_ref[i * keys : (i + 1) * keys, here]
                scores = lax.dot_general(
                    two, kp, (((1,), (1,)), ((), ())), preferred_element_type=f32
                ) * (HEAD_DIM ** -0.5)
                top = jnp.max(scores, axis=1, keepdims=True)
                raised = jnp.exp(scores - top)
                weights = raised * (1.0 / jnp.sum(raised, axis=1, keepdims=True))
                mixed = jnp.dot(weights.astype(bf16), vp, preferred_element_type=f32)
                pieces.append(jnp.where(low, mixed[:SPAN_LEN], mixed[SPAN_LEN:]).astype(bf16))
            context_rows.append(jnp.concatenate(pieces, axis=1))
        context = jnp.concatenate(context_rows, axis=0)
        total = total + lax.dot_general(
            context, weight(3, g), (((1,), (1,)), ((), ())), preferred_element_type=f32
        )
    for g in range(groups):
        out_ref[g] = total[:, g * cols : (g + 1) * cols].astype(bf16)


def attend(where, chunks, states, weights, other):
    total, width = chunks[0].shape
    spans = states.shape[0] // SPAN_LEN // weights.shape[1]
    some = total // spans
    steps = spans // SPANS_STEP
    rows = SPANS_STEP * SPAN_LEN
    last = states.shape[0] // SPAN_LEN - 1
    keys = some * len(chunks)
    groups = weights.shape[1]
    cols = width // groups

    def after(i, where_ref):
        return jnp.minimum((where_ref[0] * steps + i + 1) * SPANS_STEP, last), 0

    flops = 2 * spans * (keys * width * 2 * width + SPAN_LEN * 2 * width * width)
    return pl.pallas_call(
        attention_kernel,
        out_shape=jax.ShapeDtypeStruct((groups, spans * SPAN_LEN, cols), jnp.bfloat16),
        grid_spec=pltpu.PrefetchScalarGridSpec(
            num_scalar_prefetch=1,
            grid=(steps,),
            in_specs=[
                pl.BlockSpec((SPANS_STEP * some, width), lambda i, h: (i, 0))
                for _ in chunks
            ]
            + [
                pl.BlockSpec((rows, width), lambda i, h: (h[0] * steps + i, 0)),
                pl.BlockSpec((SPAN_LEN, width), after),
                pl.BlockSpec(memory_space=pltpu.VMEM),
                pl.BlockSpec(memory_space=pltpu.VMEM),
            ],
            out_specs=pl.BlockSpec((groups, rows, cols), lambda i, h: (0, i, 0)),
            scratch_shapes=[
                pltpu.VMEM((SPANS_STEP * keys, cols), jnp.bfloat16),
                pltpu.VMEM((SPANS_STEP * keys, cols), jnp.bfloat16),
                pltpu.VMEM((2, *weights.shape), jnp.bfloat16),
            ],
        ),
        compiler_params=pltpu.CompilerParams(
            dimension_semantics=("arbitrary",), vmem_limit_bytes=48 * 1024 * 1024
        ),
        cost_estimate=pl.CostEstimate(
            flops=flops, bytes_accessed=2 * (len(chunks) * chunks[0].size + 2 * weights.size), transcendentals=0
        ),
        name="attend",
    )(where, *chunks, states, states, weights, other)


def span_groups(peers, groups, turn):
    low = [(s // 2) % 2 == 0 for s in range(peers)]
    return [
        [s * groups + (h + (turn if low[s] else 0)) % groups for s in range(peers)]
        for h in range(groups)
    ]


def layer(
    decoder_states, encodings, neighbor_table, query_weight, key_weight, value_weight, out_weight
):
    peers = lax.axis_size(SPAN)
    groups = lax.axis_size("head")
    share = lax.axis_index(("core", "y", "x"))
    head = lax.axis_index("head")
    width = decoder_states.shape[1]

    depth = width // lax.axis_size(("core", "y", "x"))
    part = jnp.concatenate(
        [
            lax.dynamic_slice_in_dim(w, share * depth, depth, 0)
            for w in (key_weight, value_weight, query_weight)
        ]
        + [lax.dynamic_slice_in_dim(out_weight, share * depth, depth, 1).T],
        axis=1,
    )
    passed = [part]
    for step in range(1, groups):
        passed.append(lax.ppermute(part, "head", [(i, (i + step) % groups) for i in range(groups)]))
    order = (head - jnp.arange(groups, dtype=jnp.int32)) % groups
    stacked = jnp.stack(passed)[order]
    shard_ids = neighbor_table[:, :, 0].reshape(-1)
    slot_ids = neighbor_table[:, :, 1].reshape(-1)
    entries = shard_ids.shape[0]
    numbering = jnp.arange(entries, dtype=jnp.int32)
    placed = shard_ids[None, :] == numbering[:, None]
    request = jnp.sum(jnp.where(placed, slot_ids[None, :], 0), axis=1)
    wanted = lax.all_to_all(request, SPAN, split_axis=0, concat_axis=0, tiled=True)
    weights = lax.all_gather(stacked, ("y", "x"), axis=0, tiled=True)
    piece = encodings.shape[1] // CHUNKS
    pieces = encodings.reshape(-1, piece, width)
    sources = shard_ids.reshape(groups, -1)
    owned = []
    for c in range(CHUNKS):
        arrived = lax.all_to_all(
            pieces[CHUNKS * wanted + c],
            SPAN + ("head",),
            split_axis=0,
            concat_axis=0,
            axis_index_groups=span_groups(peers, groups, c % 2),
            tiled=True,
        )
        for step in range(groups):
            block = arrived[sources[(head + step) % groups]]
            if step:
                block = lax.ppermute(
                    block, "head", [(i, (i + step) % groups) for i in range(groups)]
                )
            owned.append(block.reshape(-1, width))
    weights = weights.reshape(-1, groups, depth, width)
    other = lax.ppermute(weights, "core", [(0, 1), (1, 0)])
    where = jnp.stack([head, lax.axis_index("core")])
    result = attend(where, owned, decoder_states, weights, other)
    columns = lax.all_to_all(result, "head", split_axis=0, concat_axis=0, tiled=True)
    columns = columns.reshape(decoder_states.shape[0], width // groups)
    offset = SPAN_LEN - 1
    return jnp.concatenate(
        [jnp.zeros((offset, columns.shape[1]), columns.dtype), columns[: columns.shape[0] - offset]],
        axis=0,
    )


def solution(mesh):
    fine = jax.sharding.Mesh(mesh.devices.reshape(4, 4, 2, 2, 4), SPAN + ("head",))
    return jax.shard_map(
        layer,
        mesh=fine,
        in_specs=(
            P(SPAN, None),
            P(SPAN, "head", None),
            P(SPAN, None, None),
            P(None, "head"),
            P(None, "head"),
            P(None, "head"),
            P("head", None),
        ),
        out_specs=P(SPAN, "head"),
        check_vma=False,
    )
```

```python
import jax
import jax.numpy as jnp
from jax import lax
from jax.experimental import pallas as pl
from jax.experimental.pallas import tpu as pltpu
from jax.sharding import PartitionSpec as P


HEAD_DIM = 64
SPAN_LEN = 64
SPANS_STEP = 2
CHUNKS = 2
SPAN = ("y", "x", "z", "core")


def attention_kernel(where_ref, *refs):
    x_refs = refs[:-8]
    now_ref, next_ref, own_ref, other_ref, out_ref, k_ref, v_ref, w_ref = refs[-8:]
    f32, bf16 = jnp.float32, jnp.bfloat16
    spans = SPANS_STEP
    some, width = x_refs[0].shape
    some //= spans
    keys = len(x_refs) * some
    groups = own_ref.shape[1]
    cols = width // groups

    @pl.when(pl.program_id(0) == 0)
    def _():
        core = where_ref[1]
        w_ref[core] = own_ref[...]
        w_ref[1 - core] = other_ref[...]

    rows = spans * SPAN_LEN

    x = jnp.concatenate(
        [
            x_ref[i * some : (i + 1) * some]
            for i in range(spans)
            for x_ref in x_refs
        ],
        axis=0,
    )
    both = jnp.concatenate([now_ref[...], next_ref[...]], axis=0)
    row = lax.broadcasted_iota(jnp.int32, (rows, rows + SPAN_LEN), 0)
    col = lax.broadcasted_iota(jnp.int32, (rows, rows + SPAN_LEN), 1)
    shift = jnp.where(col == row + SPAN_LEN - 1, 1.0, 0.0).astype(bf16)
    states = jnp.dot(shift, both, preferred_element_type=f32).astype(bf16)

    def weight(which, g):
        return w_ref[:, :, g, :, which * cols : (which + 1) * cols].reshape(width, cols)

    total = jnp.zeros((rows, width), f32)
    lane = lax.broadcasted_iota(jnp.int32, (SPAN_LEN, 128), 1)
    low = lane < HEAD_DIM
    for g in range(groups):
        k_ref[...] = jnp.dot(x, weight(0, g), preferred_element_type=f32).astype(bf16)
        v_ref[...] = jnp.dot(x, weight(1, g), preferred_element_type=f32).astype(bf16)
        q = jnp.dot(states, weight(2, g), preferred_element_type=f32).astype(bf16)
        context_rows = []
        for i in range(spans):
            pieces = []
            for pair in range(cols // 128):
                here = slice(pair * 128, pair * 128 + 128)
                qp = q[i * SPAN_LEN : (i + 1) * SPAN_LEN, here]
                zero = jnp.zeros_like(qp)
                two = jnp.concatenate([jnp.where(low, qp, zero), jnp.where(low, zero, qp)], axis=0)
                kp = k_ref[i * keys : (i + 1) * keys, here]
                vp = v_ref[i * keys : (i + 1) * keys, here]
                scores = lax.dot_general(
                    two, kp, (((1,), (1,)), ((), ())), preferred_element_type=f32
                ) * (HEAD_DIM ** -0.5)
                top = jnp.max(scores, axis=1, keepdims=True)
                raised = jnp.exp(scores - top)
                weights = raised * (1.0 / jnp.sum(raised, axis=1, keepdims=True))
                mixed = jnp.dot(weights.astype(bf16), vp, preferred_element_type=f32)
                pieces.append(jnp.where(low, mixed[:SPAN_LEN], mixed[SPAN_LEN:]).astype(bf16))
            context_rows.append(jnp.concatenate(pieces, axis=1))
        context = jnp.concatenate(context_rows, axis=0)
        total = total + lax.dot_general(
            context, weight(3, g), (((1,), (1,)), ((), ())), preferred_element_type=f32
        )
    for g in range(groups):
        out_ref[g] = total[:, g * cols : (g + 1) * cols].astype(bf16)


def attend(where, chunks, states, weights, other):
    total, width = chunks[0].shape
    spans = states.shape[0] // SPAN_LEN // weights.shape[1]
    some = total // spans
    steps = spans // SPANS_STEP
    rows = SPANS_STEP * SPAN_LEN
    last = states.shape[0] // SPAN_LEN - 1
    keys = some * len(chunks)
    groups = weights.shape[1]
    cols = width // groups

    def after(i, where_ref):
        return jnp.minimum((where_ref[0] * steps + i + 1) * SPANS_STEP, last), 0

    flops = 2 * spans * (keys * width * 2 * width + SPAN_LEN * 2 * width * width)
    return pl.pallas_call(
        attention_kernel,
        out_shape=jax.ShapeDtypeStruct((groups, spans * SPAN_LEN, cols), jnp.bfloat16),
        grid_spec=pltpu.PrefetchScalarGridSpec(
            num_scalar_prefetch=1,
            grid=(steps,),
            in_specs=[
                pl.BlockSpec((SPANS_STEP * some, width), lambda i, h: (i, 0))
                for _ in chunks
            ]
            + [
                pl.BlockSpec((rows, width), lambda i, h: (h[0] * steps + i, 0)),
                pl.BlockSpec((SPAN_LEN, width), after),
                pl.BlockSpec(memory_space=pltpu.VMEM),
                pl.BlockSpec(memory_space=pltpu.VMEM),
            ],
            out_specs=pl.BlockSpec((groups, rows, cols), lambda i, h: (0, i, 0)),
            scratch_shapes=[
                pltpu.VMEM((SPANS_STEP * keys, cols), jnp.bfloat16),
                pltpu.VMEM((SPANS_STEP * keys, cols), jnp.bfloat16),
                pltpu.VMEM((2, *weights.shape), jnp.bfloat16),
            ],
        ),
        compiler_params=pltpu.CompilerParams(
            dimension_semantics=("arbitrary",), vmem_limit_bytes=48 * 1024 * 1024
        ),
        cost_estimate=pl.CostEstimate(
            flops=flops, bytes_accessed=2 * (len(chunks) * chunks[0].size + 2 * weights.size), transcendentals=0
        ),
        name="attend",
    )(where, *chunks, states, states, weights, other)


def layer(
    decoder_states, encodings, neighbor_table, query_weight, key_weight, value_weight, out_weight
):
    groups = lax.axis_size("head")
    share = lax.axis_index(("core", "y", "x"))
    head = lax.axis_index("head")
    width = decoder_states.shape[1]

    depth = width // lax.axis_size(("core", "y", "x"))
    part = jnp.concatenate(
        [
            lax.dynamic_slice_in_dim(w, share * depth, depth, 0)
            for w in (key_weight, value_weight, query_weight)
        ]
        + [lax.dynamic_slice_in_dim(out_weight, share * depth, depth, 1).T],
        axis=1,
    )
    passed = [part]
    for step in range(1, groups):
        passed.append(lax.ppermute(part, "head", [(i, (i + step) % groups) for i in range(groups)]))
    order = (head - jnp.arange(groups, dtype=jnp.int32)) % groups
    stacked = jnp.stack(passed)[order]
    shard_ids = neighbor_table[:, :, 0].reshape(-1)
    slot_ids = neighbor_table[:, :, 1].reshape(-1)
    entries = shard_ids.shape[0]
    numbering = jnp.arange(entries, dtype=jnp.int32)
    placed = shard_ids[None, :] == numbering[:, None]
    request = jnp.sum(jnp.where(placed, slot_ids[None, :], 0), axis=1)
    wanted = lax.all_to_all(request, SPAN, split_axis=0, concat_axis=0, tiled=True)
    weights = lax.all_gather(stacked, ("y", "x"), axis=0, tiled=True)
    piece = encodings.shape[1] // CHUNKS
    pieces = encodings.reshape(-1, piece, width)
    sources = shard_ids.reshape(groups, -1)
    owned = []
    for c in range(CHUNKS):
        arrived = lax.all_to_all(
            pieces[CHUNKS * wanted + c],
            SPAN,
            split_axis=0,
            concat_axis=0,
            tiled=True,
        )
        for step in range(groups):
            block = arrived[sources[(head + step) % groups]]
            if step:
                block = lax.ppermute(
                    block, "head", [(i, (i + step) % groups) for i in range(groups)]
                )
            owned.append(block.reshape(-1, width))
    weights = weights.reshape(-1, groups, depth, width)
    other = lax.ppermute(weights, "core", [(0, 1), (1, 0)])
    where = jnp.stack([head, lax.axis_index("core")])
    result = attend(where, owned, decoder_states, weights, other)
    columns = lax.all_to_all(result, "head", split_axis=0, concat_axis=0, tiled=True)
    columns = columns.reshape(decoder_states.shape[0], width // groups)
    offset = SPAN_LEN - 1
    return jnp.concatenate(
        [jnp.zeros((offset, columns.shape[1]), columns.dtype), columns[: columns.shape[0] - offset]],
        axis=0,
    )


def solution(mesh):
    fine = jax.sharding.Mesh(mesh.devices.reshape(4, 4, 2, 2, 4), SPAN + ("head",))
    return jax.shard_map(
        layer,
        mesh=fine,
        in_specs=(
            P(SPAN, None),
            P(SPAN, "head", None),
            P(SPAN, None, None),
            P(None, "head"),
            P(None, "head"),
            P(None, "head"),
            P("head", None),
        ),
        out_specs=P(SPAN, "head"),
        check_vma=False,
    )
```

```python
import jax
import jax.numpy as jnp
from jax import lax
from jax.experimental import pallas as pl
from jax.experimental.pallas import tpu as pltpu
from jax.sharding import PartitionSpec as P


HEAD_DIM = 64
SPAN_LEN = 64
SPANS_STEP = 2
CHUNKS = 2
PARTS = 2
MIB = 1024 * 1024
SPAN = ("y", "x", "z", "core")


def weight_of(w_ref, which, g):
    width, cols = w_ref.shape[-1], w_ref.shape[-1] // w_ref.shape[2]
    return w_ref[:, :, g, :, which * cols : (which + 1) * cols].reshape(width, cols)


def rows_of(x_refs):
    some = x_refs[0].shape[0] // SPANS_STEP
    return jnp.concatenate(
        [x_ref[i * some : (i + 1) * some] for i in range(SPANS_STEP) for x_ref in x_refs], axis=0
    )


def prepare_kernel(where_ref, *refs):
    x_refs = refs[:-8]
    now_ref, next_ref, own_ref, other_ref, q_ref, k_ref, v_ref, w_ref = refs[-8:]
    f32, bf16 = jnp.float32, jnp.bfloat16
    groups = own_ref.shape[1]
    cols = own_ref.shape[-1] // groups
    rows = SPANS_STEP * SPAN_LEN

    @pl.when(pl.program_id(0) == 0)
    def _():
        core = where_ref[1]
        w_ref[core] = own_ref[...]
        w_ref[1 - core] = other_ref[...]

    x = rows_of(x_refs)
    both = jnp.concatenate([now_ref[...], next_ref[...]], axis=0)
    row = lax.broadcasted_iota(jnp.int32, (rows, rows + SPAN_LEN), 0)
    col = lax.broadcasted_iota(jnp.int32, (rows, rows + SPAN_LEN), 1)
    shift = jnp.where(col == row + SPAN_LEN - 1, 1.0, 0.0).astype(bf16)
    states = jnp.dot(shift, both, preferred_element_type=f32).astype(bf16)
    for g in range(groups):
        here = slice(g * cols, (g + 1) * cols)
        for source, target, which in ((x, k_ref, 0), (x, v_ref, 1), (states, q_ref, 2)):
            target[:, here] = jnp.dot(
                source, weight_of(w_ref, which, g), preferred_element_type=f32
            ).astype(bf16)


def attend_kernel(*refs):
    x_refs = refs[:-7]
    q_ref, k_ref, v_ref, w_ref, out_ref, late_k_ref, late_v_ref = refs[-7:]
    f32, bf16 = jnp.float32, jnp.bfloat16
    spans, width = SPANS_STEP, w_ref.shape[-1]
    groups = w_ref.shape[2]
    cols = width // groups
    rows = spans * SPAN_LEN
    early = k_ref.shape[0] // spans
    late = late_k_ref.shape[0] // spans
    x = rows_of(x_refs)
    total = jnp.zeros((rows, width), f32)
    lane = lax.broadcasted_iota(jnp.int32, (SPAN_LEN, 128), 1)
    low = lane < HEAD_DIM
    for g in range(groups):
        for target, which in ((late_k_ref, 0), (late_v_ref, 1)):
            target[...] = jnp.dot(
                x, weight_of(w_ref, which, g), preferred_element_type=f32
            ).astype(bf16)
        context_rows = []
        for i in range(spans):
            pieces = []
            for pair in range(cols // 128):
                here = slice(pair * 128, pair * 128 + 128)
                there = slice(g * cols + pair * 128, g * cols + pair * 128 + 128)
                first, second = slice(i * early, (i + 1) * early), slice(i * late, (i + 1) * late)
                qp = q_ref[i * SPAN_LEN : (i + 1) * SPAN_LEN, there]
                zero = jnp.zeros_like(qp)
                two = jnp.concatenate([jnp.where(low, qp, zero), jnp.where(low, zero, qp)], axis=0)
                kp = jnp.concatenate([k_ref[first, there], late_k_ref[second, here]], axis=0)
                vp = jnp.concatenate([v_ref[first, there], late_v_ref[second, here]], axis=0)
                scores = lax.dot_general(
                    two, kp, (((1,), (1,)), ((), ())), preferred_element_type=f32
                ) * (HEAD_DIM ** -0.5)
                top = jnp.max(scores, axis=1, keepdims=True)
                raised = jnp.exp(scores - top)
                weights = raised * (1.0 / jnp.sum(raised, axis=1, keepdims=True))
                mixed = jnp.dot(weights.astype(bf16), vp, preferred_element_type=f32)
                pieces.append(jnp.where(low, mixed[:SPAN_LEN], mixed[SPAN_LEN:]).astype(bf16))
            context_rows.append(jnp.concatenate(pieces, axis=1))
        context = jnp.concatenate(context_rows, axis=0)
        total = total + lax.dot_general(
            context, weight_of(w_ref, 3, g), (((1,), (1,)), ((), ())), preferred_element_type=f32
        )
    for g in range(groups):
        out_ref[g] = total[:, g * cols : (g + 1) * cols].astype(bf16)


def settings(room):
    return pltpu.CompilerParams(
        dimension_semantics=("arbitrary",), vmem_limit_bytes=room * MIB
    )


def prepare(where, chunks, states, weights, other):
    held, width = chunks[0].shape
    spans = states.shape[0] // SPAN_LEN // weights.shape[1]
    some = held // spans
    steps = spans // SPANS_STEP
    rows = SPANS_STEP * SPAN_LEN
    last = states.shape[0] // SPAN_LEN - 1
    keys = some * len(chunks)
    whole = pl.BlockSpec(memory_space=pltpu.VMEM)
    bf16 = jnp.bfloat16

    def after(i, h):
        return jnp.minimum((h[0] * steps + i + 1) * SPANS_STEP, last), 0

    return pl.pallas_call(
        prepare_kernel,
        out_shape=(
            jax.ShapeDtypeStruct((spans * SPAN_LEN, width), bf16),
            jax.ShapeDtypeStruct((spans * keys, width), bf16),
            jax.ShapeDtypeStruct((spans * keys, width), bf16),
            jax.ShapeDtypeStruct((2, *weights.shape), bf16),
        ),
        grid_spec=pltpu.PrefetchScalarGridSpec(
            num_scalar_prefetch=1,
            grid=(steps,),
            in_specs=[pl.BlockSpec((SPANS_STEP * some, width), lambda i, h: (i, 0)) for _ in chunks]
            + [
                pl.BlockSpec((rows, width), lambda i, h: (h[0] * steps + i, 0)),
                pl.BlockSpec((SPAN_LEN, width), after),
                whole,
                whole,
            ],
            out_specs=(
                pl.BlockSpec((rows, width), lambda i, h: (i, 0)),
                pl.BlockSpec((SPANS_STEP * keys, width), lambda i, h: (i, 0)),
                pl.BlockSpec((SPANS_STEP * keys, width), lambda i, h: (i, 0)),
                whole,
            ),
        ),
        compiler_params=settings(30),
        cost_estimate=pl.CostEstimate(
            flops=2 * spans * width * width * (2 * keys + SPAN_LEN),
            bytes_accessed=2 * (len(chunks) * chunks[0].size + 4 * weights.size),
            transcendentals=0,
        ),
        name="prepare",
    )(where, *chunks, states, states, weights, other)


def attend(part, chunks, queries, keys, values, weights):
    held, width = chunks[0].shape
    spans = queries.shape[0] // SPAN_LEN
    some = held // spans
    steps = spans // SPANS_STEP // PARTS
    rows = SPANS_STEP * SPAN_LEN
    early = keys.shape[0] // spans
    late = some * len(chunks)
    groups = weights.shape[2]
    cols = width // groups

    def block(count):
        return pl.BlockSpec((SPANS_STEP * count, width), lambda i: (part * steps + i, 0))

    return pl.pallas_call(
        attend_kernel,
        out_shape=jax.ShapeDtypeStruct((groups, steps * rows, cols), jnp.bfloat16),
        grid=(steps,),
        in_specs=[block(some) for _ in chunks]
        + [block(SPAN_LEN), block(early), block(early), pl.BlockSpec(memory_space=pltpu.VMEM)],
        out_specs=pl.BlockSpec((groups, rows, cols), lambda i: (0, i, 0)),
        scratch_shapes=[
            pltpu.VMEM((SPANS_STEP * late, cols), jnp.bfloat16),
            pltpu.VMEM((SPANS_STEP * late, cols), jnp.bfloat16),
        ],
        compiler_params=settings(30),
        cost_estimate=pl.CostEstimate(
            flops=2 * spans // PARTS * width * width * (2 * late + 6 * SPAN_LEN),
            bytes_accessed=2 * (len(chunks) * chunks[0].size // PARTS + weights.size),
            transcendentals=0,
        ),
    )(*chunks, queries, keys, values, weights)


def layer(
    decoder_states, encodings, neighbor_table, query_weight, key_weight, value_weight, out_weight
):
    groups = lax.axis_size("head")
    share = lax.axis_index(("core", "y", "x"))
    head = lax.axis_index("head")
    width = decoder_states.shape[1]

    depth = width // lax.axis_size(("core", "y", "x"))
    part = jnp.concatenate(
        [
            lax.dynamic_slice_in_dim(w, share * depth, depth, 0)
            for w in (key_weight, value_weight, query_weight)
        ]
        + [lax.dynamic_slice_in_dim(out_weight, share * depth, depth, 1).T],
        axis=1,
    )
    passed = [part]
    for step in range(1, groups):
        passed.append(lax.ppermute(part, "head", [(i, (i + step) % groups) for i in range(groups)]))
    order = (head - jnp.arange(groups, dtype=jnp.int32)) % groups
    stacked = jnp.stack(passed)[order]
    shard_ids = neighbor_table[:, :, 0].reshape(-1)
    slot_ids = neighbor_table[:, :, 1].reshape(-1)
    entries = shard_ids.shape[0]
    numbering = jnp.arange(entries, dtype=jnp.int32)
    placed = shard_ids[None, :] == numbering[:, None]
    request = jnp.sum(jnp.where(placed, slot_ids[None, :], 0), axis=1)
    wanted = lax.all_to_all(request, SPAN, split_axis=0, concat_axis=0, tiled=True)
    weights = lax.all_gather(stacked, ("y", "x"), axis=0, tiled=True)
    piece = encodings.shape[1] // CHUNKS
    pieces = encodings.reshape(-1, piece, width)
    sources = shard_ids.reshape(groups, -1)
    owned = []
    for c in range(CHUNKS):
        arrived = lax.all_to_all(
            pieces[CHUNKS * wanted + c],
            SPAN,
            split_axis=0,
            concat_axis=0,
            tiled=True,
        )
        for step in range(groups):
            block = arrived[sources[(head + step) % groups]]
            if step:
                block = lax.ppermute(
                    block, "head", [(i, (i + step) % groups) for i in range(groups)]
                )
            owned.append(block.reshape(-1, width))
    weights = weights.reshape(-1, groups, depth, width)
    other = lax.ppermute(weights, "core", [(0, 1), (1, 0)])
    where = jnp.stack([head, lax.axis_index("core")])
    queries, keys, values, weights = prepare(where, owned[:groups], decoder_states, weights, other)
    returned = []
    for p in range(PARTS):
        result = attend(p, owned[groups:], queries, keys, values, weights)
        returned.append(
            lax.all_to_all(result, "head", split_axis=0, concat_axis=0, tiled=True)
        )
    columns = jnp.concatenate(returned, axis=1)
    columns = columns.reshape(decoder_states.shape[0], width // groups)
    offset = SPAN_LEN - 1
    return jnp.concatenate(
        [jnp.zeros((offset, columns.shape[1]), columns.dtype), columns[: columns.shape[0] - offset]],
        axis=0,
    )


def solution(mesh):
    fine = jax.sharding.Mesh(mesh.devices.reshape(4, 4, 2, 2, 4), SPAN + ("head",))
    return jax.shard_map(
        layer,
        mesh=fine,
        in_specs=(
            P(SPAN, None),
            P(SPAN, "head", None),
            P(SPAN, None, None),
            P(None, "head"),
            P(None, "head"),
            P(None, "head"),
            P("head", None),
        ),
        out_specs=P(SPAN, "head"),
        check_vma=False,
    )
```

```python
import jax
import jax.numpy as jnp
from jax import lax
from jax.experimental import pallas as pl
from jax.experimental.pallas import tpu as pltpu
from jax.sharding import PartitionSpec as P


HEAD_DIM = 64
SPAN_LEN = 64
SPANS_STEP = 2
CHUNKS = 2
PARTS = 2
VMEM_BYTES = 62 * 1024 * 1024
SPAN = ("y", "x", "z", "core")


def weight_of(w_ref, which, g):
    width, cols = w_ref.shape[-1], w_ref.shape[-1] // w_ref.shape[2]
    return w_ref[:, :, g, :, which * cols : (which + 1) * cols].reshape(width, cols)


def rows_of(x_refs, spans):
    some = x_refs[0].shape[0] // spans
    return jnp.concatenate(
        [x_ref[i * some : (i + 1) * some] for i in range(spans) for x_ref in x_refs], axis=0
    )


def prepare_kernel(where_ref, *refs):
    x_refs = refs[:-8]
    now_ref, next_ref, own_ref, other_ref, q_ref, k_ref, v_ref, w_ref = refs[-8:]
    f32, bf16 = jnp.float32, jnp.bfloat16
    groups = own_ref.shape[1]
    cols = own_ref.shape[-1] // groups
    rows = SPANS_STEP * SPAN_LEN

    @pl.when(pl.program_id(0) == 0)
    def _():
        core = where_ref[1]
        w_ref[core] = own_ref[...]
        w_ref[1 - core] = other_ref[...]

    x = rows_of(x_refs, SPANS_STEP)
    both = jnp.concatenate([now_ref[...], next_ref[...]], axis=0)
    row = lax.broadcasted_iota(jnp.int32, (rows, rows + SPAN_LEN), 0)
    col = lax.broadcasted_iota(jnp.int32, (rows, rows + SPAN_LEN), 1)
    shift = jnp.where(col == row + SPAN_LEN - 1, 1.0, 0.0).astype(bf16)
    states = jnp.dot(shift, both, preferred_element_type=f32).astype(bf16)
    for g in range(groups):
        here = slice(g * cols, (g + 1) * cols)
        for source, target, which in ((x, k_ref, 0), (x, v_ref, 1), (states, q_ref, 2)):
            target[:, here] = jnp.dot(
                source, weight_of(w_ref, which, g), preferred_element_type=f32
            ).astype(bf16)


def attend_kernel(*refs):
    x_refs = refs[:-9]
    q_ref, k_ref, v_ref, w_ref, out_ref, x_ref, late_k_ref, late_v_ref, total_ref = refs[-9:]
    f32, bf16 = jnp.float32, jnp.bfloat16
    width, cols = x_ref.shape[1], q_ref.shape[1]
    spans = q_ref.shape[0] // SPAN_LEN
    early = k_ref.shape[0] // spans
    late = late_k_ref.shape[0] // spans
    group, groups = pl.program_id(0), width // cols
    lane = lax.broadcasted_iota(jnp.int32, (SPAN_LEN, 128), 1)
    low = lane < HEAD_DIM

    @pl.when(group == 0)
    def _():
        x_ref[...] = rows_of(x_refs, spans)
        total_ref[...] = jnp.zeros_like(total_ref)

    def weight(which):
        return w_ref[:, :, 0, :, which * cols : (which + 1) * cols].reshape(width, cols)

    for target, which in ((late_k_ref, 0), (late_v_ref, 1)):
        target[...] = jnp.dot(x_ref[...], weight(which), preferred_element_type=f32).astype(bf16)
    context_rows = []
    for i in range(spans):
        pieces = []
        first, second = slice(i * early, (i + 1) * early), slice(i * late, (i + 1) * late)
        for pair in range(cols // 128):
            here = slice(pair * 128, pair * 128 + 128)
            qp = q_ref[i * SPAN_LEN : (i + 1) * SPAN_LEN, here]
            zero = jnp.zeros_like(qp)
            two = jnp.concatenate([jnp.where(low, qp, zero), jnp.where(low, zero, qp)], axis=0)
            kp = jnp.concatenate([k_ref[first, here], late_k_ref[second, here]], axis=0)
            vp = jnp.concatenate([v_ref[first, here], late_v_ref[second, here]], axis=0)
            scores = lax.dot_general(
                two, kp, (((1,), (1,)), ((), ())), preferred_element_type=f32
            ) * (HEAD_DIM ** -0.5)
            top = jnp.max(scores, axis=1, keepdims=True)
            raised = jnp.exp(scores - top)
            weights = raised * (1.0 / jnp.sum(raised, axis=1, keepdims=True))
            mixed = jnp.dot(weights.astype(bf16), vp, preferred_element_type=f32)
            pieces.append(jnp.where(low, mixed[:SPAN_LEN], mixed[SPAN_LEN:]).astype(bf16))
        context_rows.append(jnp.concatenate(pieces, axis=1))
    context = jnp.concatenate(context_rows, axis=0)
    total_ref[...] += lax.dot_general(
        context, weight(3), (((1,), (1,)), ((), ())), preferred_element_type=f32
    )

    @pl.when(group == groups - 1)
    def _():
        for g in range(groups):
            out_ref[g] = total_ref[:, g * cols : (g + 1) * cols].astype(bf16)


def settings():
    return pltpu.CompilerParams(
        dimension_semantics=("arbitrary",), vmem_limit_bytes=VMEM_BYTES
    )


def prepare(where, chunks, states, weights, other):
    held, width = chunks[0].shape
    spans = states.shape[0] // SPAN_LEN // weights.shape[1]
    some = held // spans
    steps = spans // SPANS_STEP
    rows = SPANS_STEP * SPAN_LEN
    last = states.shape[0] // SPAN_LEN - 1
    keys = some * len(chunks)
    whole = pl.BlockSpec(memory_space=pltpu.VMEM)
    bf16 = jnp.bfloat16

    def after(i, h):
        return jnp.minimum((h[0] * steps + i + 1) * SPANS_STEP, last), 0

    return pl.pallas_call(
        prepare_kernel,
        out_shape=(
            jax.ShapeDtypeStruct((spans * SPAN_LEN, width), bf16),
            jax.ShapeDtypeStruct((spans * keys, width), bf16),
            jax.ShapeDtypeStruct((spans * keys, width), bf16),
            jax.ShapeDtypeStruct((2, *weights.shape), bf16),
        ),
        grid_spec=pltpu.PrefetchScalarGridSpec(
            num_scalar_prefetch=1,
            grid=(steps,),
            in_specs=[pl.BlockSpec((SPANS_STEP * some, width), lambda i, h: (i, 0)) for _ in chunks]
            + [
                pl.BlockSpec((rows, width), lambda i, h: (h[0] * steps + i, 0)),
                pl.BlockSpec((SPAN_LEN, width), after),
                whole,
                whole,
            ],
            out_specs=(
                pl.BlockSpec((rows, width), lambda i, h: (i, 0)),
                pl.BlockSpec((SPANS_STEP * keys, width), lambda i, h: (i, 0)),
                pl.BlockSpec((SPANS_STEP * keys, width), lambda i, h: (i, 0)),
                whole,
            ),
        ),
        compiler_params=settings(),
        cost_estimate=pl.CostEstimate(
            flops=2 * spans * width * width * (2 * keys + SPAN_LEN),
            bytes_accessed=2 * (len(chunks) * chunks[0].size + 4 * weights.size),
            transcendentals=0,
        ),
        name="prepare",
    )(where, *chunks, states, states, weights, other)


def attend(part, chunks, queries, keys, values, weights):
    held, width = chunks[0].shape
    here = queries.shape[0] // SPAN_LEN // PARTS
    some = held // PARTS
    rows = here * SPAN_LEN
    early = keys.shape[0] // PARTS
    late = some * len(chunks)
    groups = weights.shape[2]
    cols = width // groups

    def columns(count):
        return pl.BlockSpec((count, cols), lambda g: (part, g))

    return pl.pallas_call(
        attend_kernel,
        out_shape=jax.ShapeDtypeStruct((groups, rows, cols), jnp.bfloat16),
        grid=(groups,),
        in_specs=[pl.BlockSpec((some, width), lambda g: (part, 0)) for _ in chunks]
        + [
            columns(rows),
            columns(early),
            columns(early),
            pl.BlockSpec(weights.shape[:2] + (1,) + weights.shape[3:], lambda g: (0, 0, g, 0, 0)),
        ],
        out_specs=pl.BlockSpec((groups, rows, cols), lambda g: (0, 0, 0)),
        scratch_shapes=[
            pltpu.VMEM((late, width), jnp.bfloat16),
            pltpu.VMEM((late, cols), jnp.bfloat16),
            pltpu.VMEM((late, cols), jnp.bfloat16),
            pltpu.VMEM((rows, width), jnp.float32),
        ],
        compiler_params=settings(),
        cost_estimate=pl.CostEstimate(
            flops=2 * width * width * (2 * late + 6 * rows),
            bytes_accessed=2 * (late * width + weights.size),
            transcendentals=0,
        ),
    )(*chunks, queries, keys, values, weights)


def layer(
    decoder_states, encodings, neighbor_table, query_weight, key_weight, value_weight, out_weight
):
    groups = lax.axis_size("head")
    share = lax.axis_index(("core", "y", "x"))
    head = lax.axis_index("head")
    width = decoder_states.shape[1]

    depth = width // lax.axis_size(("core", "y", "x"))
    part = jnp.concatenate(
        [
            lax.dynamic_slice_in_dim(w, share * depth, depth, 0)
            for w in (key_weight, value_weight, query_weight)
        ]
        + [lax.dynamic_slice_in_dim(out_weight, share * depth, depth, 1).T],
        axis=1,
    )
    passed = [part]
    for step in range(1, groups):
        passed.append(lax.ppermute(part, "head", [(i, (i + step) % groups) for i in range(groups)]))
    order = (head - jnp.arange(groups, dtype=jnp.int32)) % groups
    stacked = jnp.stack(passed)[order]
    shard_ids = neighbor_table[:, :, 0].reshape(-1)
    slot_ids = neighbor_table[:, :, 1].reshape(-1)
    entries = shard_ids.shape[0]
    numbering = jnp.arange(entries, dtype=jnp.int32)
    placed = shard_ids[None, :] == numbering[:, None]
    request = jnp.sum(jnp.where(placed, slot_ids[None, :], 0), axis=1)
    wanted = lax.all_to_all(request, SPAN, split_axis=0, concat_axis=0, tiled=True)
    weights = lax.all_gather(stacked, ("y", "x"), axis=0, tiled=True)
    piece = encodings.shape[1] // CHUNKS
    pieces = encodings.reshape(-1, piece, width)
    sources = shard_ids.reshape(groups, -1)
    owned = []
    for c in range(CHUNKS):
        arrived = lax.all_to_all(
            pieces[CHUNKS * wanted + c],
            SPAN,
            split_axis=0,
            concat_axis=0,
            tiled=True,
        )
        for step in range(groups):
            block = arrived[sources[(head + step) % groups]]
            if step:
                block = lax.ppermute(
                    block, "head", [(i, (i + step) % groups) for i in range(groups)]
                )
            owned.append(block.reshape(-1, width))
    weights = weights.reshape(-1, groups, depth, width)
    other = lax.ppermute(weights, "core", [(0, 1), (1, 0)])
    where = jnp.stack([head, lax.axis_index("core")])
    queries, keys, values, weights = prepare(where, owned[:groups], decoder_states, weights, other)
    returned = []
    for p in range(PARTS):
        result = attend(p, owned[groups:], queries, keys, values, weights)
        returned.append(
            lax.all_to_all(result, "head", split_axis=0, concat_axis=0, tiled=True)
        )
    columns = jnp.concatenate(returned, axis=1)
    columns = columns.reshape(decoder_states.shape[0], width // groups)
    offset = SPAN_LEN - 1
    return jnp.concatenate(
        [jnp.zeros((offset, columns.shape[1]), columns.dtype), columns[: columns.shape[0] - offset]],
        axis=0,
    )


def solution(mesh):
    fine = jax.sharding.Mesh(mesh.devices.reshape(4, 4, 2, 2, 4), SPAN + ("head",))
    return jax.shard_map(
        layer,
        mesh=fine,
        in_specs=(
            P(SPAN, None),
            P(SPAN, "head", None),
            P(SPAN, None, None),
            P(None, "head"),
            P(None, "head"),
            P(None, "head"),
            P("head", None),
        ),
        out_specs=P(SPAN, "head"),
        check_vma=False,
    )
```

```python
import jax
import jax.numpy as jnp
from jax import lax
from jax.experimental import pallas as pl
from jax.experimental.pallas import tpu as pltpu
from jax.sharding import PartitionSpec as P


HEAD_DIM = 64
SPAN_LEN = 64
SPANS_STEP = 2
CHUNKS = 2
PARTS = 2
VMEM_BYTES = 62 * 1024 * 1024
SPAN = ("y", "x", "z", "core")


def weight_of(w_ref, which, g):
    width, cols = w_ref.shape[-1], w_ref.shape[-1] // w_ref.shape[2]
    return w_ref[:, :, g, :, which * cols : (which + 1) * cols].reshape(width, cols)


def rows_of(x_refs, spans):
    some = x_refs[0].shape[0] // spans
    return jnp.concatenate(
        [x_ref[i * some : (i + 1) * some] for i in range(spans) for x_ref in x_refs], axis=0
    )


def prepare_kernel(where_ref, *refs):
    x_refs = refs[:-8]
    now_ref, next_ref, own_ref, other_ref, q_ref, k_ref, v_ref, w_ref = refs[-8:]
    f32, bf16 = jnp.float32, jnp.bfloat16
    groups = own_ref.shape[1]
    cols = own_ref.shape[-1] // groups
    rows = SPANS_STEP * SPAN_LEN

    @pl.when(pl.program_id(0) == 0)
    def _():
        core = where_ref[1]
        w_ref[core] = own_ref[...]
        w_ref[1 - core] = other_ref[...]

    x = rows_of(x_refs, SPANS_STEP)
    both = jnp.concatenate([now_ref[...], next_ref[...]], axis=0)
    row = lax.broadcasted_iota(jnp.int32, (rows, rows + SPAN_LEN), 0)
    col = lax.broadcasted_iota(jnp.int32, (rows, rows + SPAN_LEN), 1)
    shift = jnp.where(col == row + SPAN_LEN - 1, 1.0, 0.0).astype(bf16)
    states = jnp.dot(shift, both, preferred_element_type=f32).astype(bf16)
    for g in range(groups):
        here = slice(g * cols, (g + 1) * cols)
        for source, target, which in ((x, k_ref, 0), (x, v_ref, 1), (states, q_ref, 2)):
            target[:, here] = jnp.dot(
                source, weight_of(w_ref, which, g), preferred_element_type=f32
            ).astype(bf16)


def attend_kernel(*refs):
    x_refs = refs[:-9]
    q_ref, k_ref, v_ref, w_ref, out_ref, x_ref, late_k_ref, late_v_ref, total_ref = refs[-9:]
    f32, bf16 = jnp.float32, jnp.bfloat16
    width, cols = x_ref.shape[1], q_ref.shape[1]
    spans = q_ref.shape[0] // SPAN_LEN
    early = k_ref.shape[0] // spans
    late = late_k_ref.shape[0] // spans
    group, groups = pl.program_id(0), width // cols
    lane = lax.broadcasted_iota(jnp.int32, (SPAN_LEN, 128), 1)
    low = lane < HEAD_DIM

    @pl.when(group == 0)
    def _():
        x_ref[...] = rows_of(x_refs, spans)
        total_ref[...] = jnp.zeros_like(total_ref)

    def weight(which):
        return w_ref[:, :, 0, :, which * cols : (which + 1) * cols].reshape(width, cols)

    for target, which in ((late_k_ref, 0), (late_v_ref, 1)):
        target[...] = jnp.dot(x_ref[...], weight(which), preferred_element_type=f32).astype(bf16)
    context_rows = []
    for i in range(spans):
        pieces = []
        first, second = slice(i * early, (i + 1) * early), slice(i * late, (i + 1) * late)
        for pair in range(cols // 128):
            here = slice(pair * 128, pair * 128 + 128)
            qp = q_ref[i * SPAN_LEN : (i + 1) * SPAN_LEN, here]
            zero = jnp.zeros_like(qp)
            two = jnp.concatenate([jnp.where(low, qp, zero), jnp.where(low, zero, qp)], axis=0)
            kp = jnp.concatenate([k_ref[first, here], late_k_ref[second, here]], axis=0)
            vp = jnp.concatenate([v_ref[first, here], late_v_ref[second, here]], axis=0)
            scores = lax.dot_general(
                two, kp, (((1,), (1,)), ((), ())), preferred_element_type=f32
            ) * (HEAD_DIM ** -0.5)
            top = jnp.max(scores, axis=1, keepdims=True)
            raised = jnp.exp(scores - top)
            weights = raised * (1.0 / jnp.sum(raised, axis=1, keepdims=True))
            mixed = jnp.dot(weights.astype(bf16), vp, preferred_element_type=f32)
            pieces.append(jnp.where(low, mixed[:SPAN_LEN], mixed[SPAN_LEN:]).astype(bf16))
        context_rows.append(jnp.concatenate(pieces, axis=1))
    context = jnp.concatenate(context_rows, axis=0)
    total_ref[...] += lax.dot_general(
        context, weight(3), (((1,), (1,)), ((), ())), preferred_element_type=f32
    )

    @pl.when(group == groups - 1)
    def _():
        for g in range(groups):
            out_ref[g] = total_ref[:, g * cols : (g + 1) * cols].astype(bf16)


def settings():
    return pltpu.CompilerParams(
        dimension_semantics=("arbitrary",), vmem_limit_bytes=VMEM_BYTES
    )


def prepare(where, chunks, states, weights, other):
    held, width = chunks[0].shape
    spans = states.shape[0] // SPAN_LEN // weights.shape[1]
    some = held // spans
    steps = spans // SPANS_STEP
    rows = SPANS_STEP * SPAN_LEN
    last = states.shape[0] // SPAN_LEN - 1
    keys = some * len(chunks)
    whole = pl.BlockSpec(memory_space=pltpu.VMEM)
    bf16 = jnp.bfloat16

    def after(i, h):
        return jnp.minimum((h[0] * steps + i + 1) * SPANS_STEP, last), 0

    return pl.pallas_call(
        prepare_kernel,
        out_shape=(
            jax.ShapeDtypeStruct((spans * SPAN_LEN, width), bf16),
            jax.ShapeDtypeStruct((spans * keys, width), bf16),
            jax.ShapeDtypeStruct((spans * keys, width), bf16),
            jax.ShapeDtypeStruct((2, *weights.shape), bf16),
        ),
        grid_spec=pltpu.PrefetchScalarGridSpec(
            num_scalar_prefetch=1,
            grid=(steps,),
            in_specs=[pl.BlockSpec((SPANS_STEP * some, width), lambda i, h: (i, 0)) for _ in chunks]
            + [
                pl.BlockSpec((rows, width), lambda i, h: (h[0] * steps + i, 0)),
                pl.BlockSpec((SPAN_LEN, width), after),
                whole,
                whole,
            ],
            out_specs=(
                pl.BlockSpec((rows, width), lambda i, h: (i, 0)),
                pl.BlockSpec((SPANS_STEP * keys, width), lambda i, h: (i, 0)),
                pl.BlockSpec((SPANS_STEP * keys, width), lambda i, h: (i, 0)),
                whole,
            ),
        ),
        compiler_params=settings(),
        cost_estimate=pl.CostEstimate(
            flops=2 * spans * width * width * (2 * keys + SPAN_LEN),
            bytes_accessed=2 * (len(chunks) * chunks[0].size + 4 * weights.size),
            transcendentals=0,
        ),
        name="prepare",
    )(where, *chunks, states, states, weights, other)


def attend(part, chunks, queries, keys, values, weights):
    held, width = chunks[0].shape
    here = queries.shape[0] // SPAN_LEN // PARTS
    some = held // PARTS
    rows = here * SPAN_LEN
    early = keys.shape[0] // PARTS
    late = some * len(chunks)
    groups = weights.shape[2]
    cols = width // groups

    def columns(count):
        return pl.BlockSpec((count, cols), lambda g: (part, g))

    return pl.pallas_call(
        attend_kernel,
        out_shape=jax.ShapeDtypeStruct((groups, rows, cols), jnp.bfloat16),
        grid=(groups,),
        in_specs=[pl.BlockSpec((some, width), lambda g: (part, 0)) for _ in chunks]
        + [
            columns(rows),
            columns(early),
            columns(early),
            pl.BlockSpec(weights.shape[:2] + (1,) + weights.shape[3:], lambda g: (0, 0, g, 0, 0)),
        ],
        out_specs=pl.BlockSpec((groups, rows, cols), lambda g: (0, 0, 0)),
        scratch_shapes=[
            pltpu.VMEM((late, width), jnp.bfloat16),
            pltpu.VMEM((late, cols), jnp.bfloat16),
            pltpu.VMEM((late, cols), jnp.bfloat16),
            pltpu.VMEM((rows, width), jnp.float32),
        ],
        compiler_params=settings(),
        cost_estimate=pl.CostEstimate(
            flops=2 * width * width * (2 * late + 6 * rows),
            bytes_accessed=2 * (late * width + weights.size),
            transcendentals=0,
        ),
    )(*chunks, queries, keys, values, weights)


def layer(
    decoder_states, encodings, neighbor_table, query_weight, key_weight, value_weight, out_weight
):
    groups = lax.axis_size("head")
    share = lax.axis_index(("core", "y", "x"))
    head = lax.axis_index("head")
    width = decoder_states.shape[1]

    depth = width // lax.axis_size(("core", "y", "x"))
    part = jnp.concatenate(
        [
            lax.dynamic_slice_in_dim(w, share * depth, depth, 0)
            for w in (key_weight, value_weight, query_weight)
        ]
        + [lax.dynamic_slice_in_dim(out_weight, share * depth, depth, 1).T],
        axis=1,
    )
    passed = [part]
    for step in range(1, groups):
        passed.append(lax.ppermute(part, "head", [(i, (i + step) % groups) for i in range(groups)]))
    order = (head - jnp.arange(groups, dtype=jnp.int32)) % groups
    stacked = jnp.stack(passed)[order]
    shard_ids = neighbor_table[:, :, 0].reshape(-1)
    slot_ids = neighbor_table[:, :, 1].reshape(-1)
    entries = shard_ids.shape[0]
    numbering = jnp.arange(entries, dtype=jnp.int32)
    placed = shard_ids[None, :] == numbering[:, None]
    request = jnp.sum(jnp.where(placed, slot_ids[None, :], 0), axis=1)
    wanted = lax.all_to_all(request, SPAN, split_axis=0, concat_axis=0, tiled=True)
    weights = lax.all_gather(stacked, ("y", "x"), axis=0, tiled=True)
    piece = encodings.shape[1] // CHUNKS
    pieces = encodings.reshape(-1, piece, width)
    sources = shard_ids.reshape(groups, -1)
    flat = ("y", "x", "core")
    z = lax.axis_index("z")
    depth_y, depth_x, depth_z, cores = (lax.axis_size(axis) for axis in SPAN)
    by_plane = wanted.reshape(depth_y, depth_x, depth_z, cores).transpose(2, 0, 1, 3)
    by_plane = by_plane.reshape(depth_z, -1)
    staying, leaving = by_plane[z], by_plane[1 - z]
    sources = (
        sources // 4 * 2
        + sources % 2
        + jnp.where(sources // 2 % 2 == z, 0, by_plane.shape[1])
    )
    crossings = (
        [(p * groups + h, (1 - p) * groups + h) for p in (0, 1) for h in range(groups)],
        [
            (p * groups + h, (1 - p) * groups + (h + (1 if p else -1)) % groups)
            for p in (0, 1)
            for h in range(groups)
        ],
    )

    def exchange(block):
        return lax.all_to_all(block, flat, split_axis=0, concat_axis=0, tiled=True)

    owned = []
    for c in range(CHUNKS):
        crossed = lax.ppermute(
            pieces[CHUNKS * leaving + c], ("z", "head"), crossings[c % 2]
        )
        same = exchange(pieces[CHUNKS * staying + c])
        other = exchange(crossed)
        arrived = jnp.concatenate([same, other], axis=0)
        for step in range(groups):
            block = arrived[sources[(head + step) % groups]]
            if step:
                block = lax.ppermute(
                    block, "head", [(i, (i + step) % groups) for i in range(groups)]
                )
            owned.append(block.reshape(-1, width))
    weights = weights.reshape(-1, groups, depth, width)
    other = lax.ppermute(weights, "core", [(0, 1), (1, 0)])
    where = jnp.stack([head, lax.axis_index("core")])
    queries, keys, values, weights = prepare(where, owned[:groups], decoder_states, weights, other)
    returned = []
    for p in range(PARTS):
        result = attend(p, owned[groups:], queries, keys, values, weights)
        returned.append(
            lax.all_to_all(result, "head", split_axis=0, concat_axis=0, tiled=True)
        )
    columns = jnp.concatenate(returned, axis=1)
    columns = columns.reshape(decoder_states.shape[0], width // groups)
    offset = SPAN_LEN - 1
    return jnp.concatenate(
        [jnp.zeros((offset, columns.shape[1]), columns.dtype), columns[: columns.shape[0] - offset]],
        axis=0,
    )


def solution(mesh):
    fine = jax.sharding.Mesh(mesh.devices.reshape(4, 4, 2, 2, 4), SPAN + ("head",))
    return jax.shard_map(
        layer,
        mesh=fine,
        in_specs=(
            P(SPAN, None),
            P(SPAN, "head", None),
            P(SPAN, None, None),
            P(None, "head"),
            P(None, "head"),
            P(None, "head"),
            P("head", None),
        ),
        out_specs=P(SPAN, "head"),
        check_vma=False,
    )
```

```python
import jax
import jax.numpy as jnp
from jax import lax
from jax.experimental import pallas as pl
from jax.experimental.pallas import tpu as pltpu
from jax.sharding import PartitionSpec as P


HEAD_DIM = 64
SPAN_LEN = 64
SPANS_STEP = 2
CHUNKS = 2
PARTS = 2
VMEM_BYTES = 62 * 1024 * 1024
SPAN = ("y", "x", "z", "core")


def weight_of(w_ref, which, g):
    width, cols = w_ref.shape[-1], w_ref.shape[-1] // w_ref.shape[2]
    return w_ref[:, :, g, :, which * cols : (which + 1) * cols].reshape(width, cols)


def rows_of(x_refs, spans):
    some = x_refs[0].shape[0] // spans
    return jnp.concatenate(
        [x_ref[i * some : (i + 1) * some] for i in range(spans) for x_ref in x_refs], axis=0
    )


def prepare_kernel(where_ref, *refs):
    x_refs = refs[:-8]
    now_ref, next_ref, own_ref, other_ref, q_ref, k_ref, v_ref, w_ref = refs[-8:]
    f32, bf16 = jnp.float32, jnp.bfloat16
    groups = own_ref.shape[1]
    cols = own_ref.shape[-1] // groups
    rows = SPANS_STEP * SPAN_LEN

    @pl.when(pl.program_id(0) == 0)
    def _():
        core = where_ref[1]
        w_ref[core] = own_ref[...]
        w_ref[1 - core] = other_ref[...]

    x = rows_of(x_refs, SPANS_STEP)
    both = jnp.concatenate([now_ref[...], next_ref[...]], axis=0)
    row = lax.broadcasted_iota(jnp.int32, (rows, rows + SPAN_LEN), 0)
    col = lax.broadcasted_iota(jnp.int32, (rows, rows + SPAN_LEN), 1)
    shift = jnp.where(col == row + SPAN_LEN - 1, 1.0, 0.0).astype(bf16)
    states = jnp.dot(shift, both, preferred_element_type=f32).astype(bf16)
    for g in range(groups):
        here = slice(g * cols, (g + 1) * cols)
        for source, target, which in ((x, k_ref, 0), (x, v_ref, 1), (states, q_ref, 2)):
            target[:, here] = jnp.dot(
                source, weight_of(w_ref, which, g), preferred_element_type=f32
            ).astype(bf16)


def attend_kernel(*refs):
    x_refs = refs[:-9]
    q_ref, k_ref, v_ref, w_ref, out_ref, x_ref, late_k_ref, late_v_ref, total_ref = refs[-9:]
    f32, bf16 = jnp.float32, jnp.bfloat16
    width, cols = x_ref.shape[1], q_ref.shape[1]
    spans = q_ref.shape[0] // SPAN_LEN
    early = k_ref.shape[0] // spans
    late = late_k_ref.shape[0] // spans
    group, groups = pl.program_id(0), width // cols
    lane = lax.broadcasted_iota(jnp.int32, (SPAN_LEN, 128), 1)
    low = lane < HEAD_DIM

    @pl.when(group == 0)
    def _():
        x_ref[...] = rows_of(x_refs, spans)
        total_ref[...] = jnp.zeros_like(total_ref)

    def weight(which):
        return w_ref[:, :, 0, :, which * cols : (which + 1) * cols].reshape(width, cols)

    for target, which in ((late_k_ref, 0), (late_v_ref, 1)):
        target[...] = jnp.dot(x_ref[...], weight(which), preferred_element_type=f32).astype(bf16)
    context_rows = []
    for i in range(spans):
        pieces = []
        first, second = slice(i * early, (i + 1) * early), slice(i * late, (i + 1) * late)
        for pair in range(cols // 128):
            here = slice(pair * 128, pair * 128 + 128)
            qp = q_ref[i * SPAN_LEN : (i + 1) * SPAN_LEN, here]
            zero = jnp.zeros_like(qp)
            two = jnp.concatenate([jnp.where(low, qp, zero), jnp.where(low, zero, qp)], axis=0)
            kp = jnp.concatenate([k_ref[first, here], late_k_ref[second, here]], axis=0)
            vp = jnp.concatenate([v_ref[first, here], late_v_ref[second, here]], axis=0)
            scores = lax.dot_general(
                two, kp, (((1,), (1,)), ((), ())), preferred_element_type=f32
            ) * (HEAD_DIM ** -0.5)
            top = jnp.max(scores, axis=1, keepdims=True)
            raised = jnp.exp(scores - top)
            weights = raised * (1.0 / jnp.sum(raised, axis=1, keepdims=True))
            mixed = jnp.dot(weights.astype(bf16), vp, preferred_element_type=f32)
            pieces.append(jnp.where(low, mixed[:SPAN_LEN], mixed[SPAN_LEN:]).astype(bf16))
        context_rows.append(jnp.concatenate(pieces, axis=1))
    context = jnp.concatenate(context_rows, axis=0)
    total_ref[...] += lax.dot_general(
        context, weight(3), (((1,), (1,)), ((), ())), preferred_element_type=f32
    )

    @pl.when(group == groups - 1)
    def _():
        for g in range(groups):
            out_ref[g] = total_ref[:, g * cols : (g + 1) * cols].astype(bf16)


def settings():
    return pltpu.CompilerParams(
        dimension_semantics=("arbitrary",), vmem_limit_bytes=VMEM_BYTES
    )


def prepare(where, chunks, states, weights, other):
    held, width = chunks[0].shape
    spans = states.shape[0] // SPAN_LEN // weights.shape[1]
    some = held // spans
    steps = spans // SPANS_STEP
    rows = SPANS_STEP * SPAN_LEN
    last = states.shape[0] // SPAN_LEN - 1
    keys = some * len(chunks)
    whole = pl.BlockSpec(memory_space=pltpu.VMEM)
    bf16 = jnp.bfloat16

    def after(i, h):
        return jnp.minimum((h[0] * steps + i + 1) * SPANS_STEP, last), 0

    return pl.pallas_call(
        prepare_kernel,
        out_shape=(
            jax.ShapeDtypeStruct((spans * SPAN_LEN, width), bf16),
            jax.ShapeDtypeStruct((spans * keys, width), bf16),
            jax.ShapeDtypeStruct((spans * keys, width), bf16),
            jax.ShapeDtypeStruct((2, *weights.shape), bf16),
        ),
        grid_spec=pltpu.PrefetchScalarGridSpec(
            num_scalar_prefetch=1,
            grid=(steps,),
            in_specs=[pl.BlockSpec((SPANS_STEP * some, width), lambda i, h: (i, 0)) for _ in chunks]
            + [
                pl.BlockSpec((rows, width), lambda i, h: (h[0] * steps + i, 0)),
                pl.BlockSpec((SPAN_LEN, width), after),
                whole,
                whole,
            ],
            out_specs=(
                pl.BlockSpec((rows, width), lambda i, h: (i, 0)),
                pl.BlockSpec((SPANS_STEP * keys, width), lambda i, h: (i, 0)),
                pl.BlockSpec((SPANS_STEP * keys, width), lambda i, h: (i, 0)),
                whole,
            ),
        ),
        compiler_params=settings(),
        cost_estimate=pl.CostEstimate(
            flops=2 * spans * width * width * (2 * keys + SPAN_LEN),
            bytes_accessed=2 * (len(chunks) * chunks[0].size + 4 * weights.size),
            transcendentals=0,
        ),
        name="prepare",
    )(where, *chunks, states, states, weights, other)


def attend(part, chunks, queries, keys, values, weights):
    held, width = chunks[0].shape
    here = queries.shape[0] // SPAN_LEN // PARTS
    some = held
    rows = here * SPAN_LEN
    early = keys.shape[0] // PARTS
    late = some * len(chunks)
    groups = weights.shape[2]
    cols = width // groups

    def columns(count):
        return pl.BlockSpec((count, cols), lambda g: (part, g))

    return pl.pallas_call(
        attend_kernel,
        out_shape=jax.ShapeDtypeStruct((groups, rows, cols), jnp.bfloat16),
        grid=(groups,),
        in_specs=[pl.BlockSpec((some, width), lambda g: (0, 0)) for _ in chunks]
        + [
            columns(rows),
            columns(early),
            columns(early),
            pl.BlockSpec(weights.shape[:2] + (1,) + weights.shape[3:], lambda g: (0, 0, g, 0, 0)),
        ],
        out_specs=pl.BlockSpec((groups, rows, cols), lambda g: (0, 0, 0)),
        scratch_shapes=[
            pltpu.VMEM((late, width), jnp.bfloat16),
            pltpu.VMEM((late, cols), jnp.bfloat16),
            pltpu.VMEM((late, cols), jnp.bfloat16),
            pltpu.VMEM((rows, width), jnp.float32),
        ],
        compiler_params=settings(),
        cost_estimate=pl.CostEstimate(
            flops=2 * width * width * (2 * late + 6 * rows),
            bytes_accessed=2 * (late * width + weights.size),
            transcendentals=0,
        ),
    )(*chunks, queries, keys, values, weights)


def layer(
    decoder_states, encodings, neighbor_table, query_weight, key_weight, value_weight, out_weight
):
    groups = lax.axis_size("head")
    share = lax.axis_index(("core", "y", "x"))
    head = lax.axis_index("head")
    width = decoder_states.shape[1]

    depth = width // lax.axis_size(("core", "y", "x"))
    part = jnp.concatenate(
        [
            lax.dynamic_slice_in_dim(w, share * depth, depth, 0)
            for w in (key_weight, value_weight, query_weight)
        ]
        + [lax.dynamic_slice_in_dim(out_weight, share * depth, depth, 1).T],
        axis=1,
    )
    passed = [part]
    for step in range(1, groups):
        passed.append(lax.ppermute(part, "head", [(i, (i + step) % groups) for i in range(groups)]))
    order = (head - jnp.arange(groups, dtype=jnp.int32)) % groups
    stacked = jnp.stack(passed)[order]
    shard_ids = neighbor_table[:, :, 0].reshape(-1)
    slot_ids = neighbor_table[:, :, 1].reshape(-1)
    entries = shard_ids.shape[0]
    numbering = jnp.arange(entries, dtype=jnp.int32)
    placed = shard_ids[None, :] == numbering[:, None]
    request = jnp.sum(jnp.where(placed, slot_ids[None, :], 0), axis=1)
    wanted = lax.all_to_all(request, SPAN, split_axis=0, concat_axis=0, tiled=True)
    weights = lax.all_gather(stacked, ("y", "x"), axis=0, tiled=True)
    piece = encodings.shape[1] // CHUNKS
    pieces = encodings.reshape(-1, piece, width)
    sources = shard_ids.reshape(groups, -1)
    flat = ("y", "x", "core")
    z = lax.axis_index("z")
    depth_y, depth_x, depth_z, cores = (lax.axis_size(axis) for axis in SPAN)
    by_plane = wanted.reshape(depth_y, depth_x, depth_z, cores).transpose(2, 0, 1, 3)
    by_plane = by_plane.reshape(depth_z, -1)
    staying, leaving = by_plane[z], by_plane[1 - z]
    sources = (
        sources // 4 * 2
        + sources % 2
        + jnp.where(sources // 2 % 2 == z, 0, by_plane.shape[1])
    )
    crossings = (
        [(p * groups + h, (1 - p) * groups + h) for p in (0, 1) for h in range(groups)],
        [
            (p * groups + h, (1 - p) * groups + (h + (1 if p else -1)) % groups)
            for p in (0, 1)
            for h in range(groups)
        ],
    )

    def exchange(block):
        return lax.all_to_all(block, flat, split_axis=0, concat_axis=0, tiled=True)

    owned = []
    for c in range(CHUNKS):
        crossed = lax.ppermute(
            pieces[CHUNKS * leaving + c], ("z", "head"), crossings[c % 2]
        )
        same = exchange(pieces[CHUNKS * staying + c])
        other = exchange(crossed)
        arrived = jnp.concatenate([same, other], axis=0)
        whole = c < CHUNKS - 1
        for p in range(1 if whole else PARTS):
            taken = sources if whole else jnp.split(sources, PARTS, axis=1)[p]
            blocks = []
            for step in range(groups):
                block = arrived[taken[(head + step) % groups]]
                if step:
                    block = lax.ppermute(
                        block, "head", [(i, (i + step) % groups) for i in range(groups)]
                    )
                blocks.append(block.reshape(-1, width))
            owned.append(blocks)
    weights = weights.reshape(-1, groups, depth, width)
    other = lax.ppermute(weights, "core", [(0, 1), (1, 0)])
    where = jnp.stack([head, lax.axis_index("core")])
    queries, keys, values, weights = prepare(
        where, owned[0], decoder_states, weights, other
    )
    returned = []
    for p in range(PARTS):
        result = attend(p, owned[1 + p], queries, keys, values, weights)
        returned.append(
            lax.all_to_all(result, "head", split_axis=0, concat_axis=0, tiled=True)
        )
    columns = jnp.concatenate(returned, axis=1)
    columns = columns.reshape(decoder_states.shape[0], width // groups)
    offset = SPAN_LEN - 1
    return jnp.concatenate(
        [jnp.zeros((offset, columns.shape[1]), columns.dtype), columns[: columns.shape[0] - offset]],
        axis=0,
    )


def solution(mesh):
    fine = jax.sharding.Mesh(mesh.devices.reshape(4, 4, 2, 2, 4), SPAN + ("head",))
    return jax.shard_map(
        layer,
        mesh=fine,
        in_specs=(
            P(SPAN, None),
            P(SPAN, "head", None),
            P(SPAN, None, None),
            P(None, "head"),
            P(None, "head"),
            P(None, "head"),
            P("head", None),
        ),
        out_specs=P(SPAN, "head"),
        check_vma=False,
    )
```

```python
import jax
import jax.numpy as jnp
from jax import lax
from jax.experimental import pallas as pl
from jax.experimental.pallas import tpu as pltpu
from jax.sharding import PartitionSpec as P


HEAD_DIM = 64
SPAN_LEN = 64
SPANS_STEP = 2
CHUNKS = 2
PARTS = 2
VMEM_BYTES = 62 * 1024 * 1024
SPAN = ("y", "x", "z", "core")


def rows_of(x_refs, spans):
    some = x_refs[0].shape[0] // spans
    return jnp.concatenate(
        [x_ref[i * some : (i + 1) * some] for i in range(spans) for x_ref in x_refs], axis=0
    )


def prepare_kernel(where_ref, *refs):
    x_refs = refs[:-11]
    now_ref, next_ref, own_ref, other_ref = refs[-11:-7]
    q_ref, k_ref, v_ref, w_ref, x_ref, states_ref, last_ref = refs[-7:]
    f32, bf16 = jnp.float32, jnp.bfloat16
    width, cols = x_ref.shape[1], q_ref.shape[1]
    spans = q_ref.shape[0] // SPAN_LEN
    rows = SPANS_STEP * SPAN_LEN

    @pl.when(pl.program_id(0) == 0)
    def _():
        x_ref[...] = rows_of(x_refs, spans)
        row = lax.broadcasted_iota(jnp.int32, (rows, rows + SPAN_LEN), 0)
        col = lax.broadcasted_iota(jnp.int32, (rows, rows + SPAN_LEN), 1)
        shift = jnp.where(col == row + SPAN_LEN - 1, 1.0, 0.0).astype(bf16)
        for first in range(0, spans * SPAN_LEN, rows):
            if first + rows < spans * SPAN_LEN:
                both = now_ref[first : first + rows + SPAN_LEN]
            else:
                both = jnp.concatenate([now_ref[first:], next_ref[...]], axis=0)
            states_ref[first : first + rows] = jnp.dot(
                shift, both, preferred_element_type=f32
            ).astype(bf16)

    core = where_ref[1]
    for slot, ref in ((core, own_ref), (1 - core, other_ref)):
        w_ref[slot] = ref[:, :, :, : 2 * cols]
        last_ref[slot] = ref[:, :, :, 2 * cols :]
    for source, target, held_ref, first in (
        (x_ref, k_ref, w_ref, 0),
        (x_ref, v_ref, w_ref, cols),
        (states_ref, q_ref, last_ref, 0),
    ):
        weight = held_ref[:, :, 0, :, first : first + cols].reshape(width, cols)
        target[...] = jnp.dot(source[...], weight, preferred_element_type=f32).astype(bf16)


def attend_kernel(where_ref, *refs):
    x_refs = refs[:-12]
    q_ref, k_ref, v_ref, w_ref, own_ref, other_ref, out_ref = refs[-12:-5]
    x_ref, late_k_ref, late_v_ref, total_ref, last_ref = refs[-5:]
    f32, bf16 = jnp.float32, jnp.bfloat16
    width, cols = x_ref.shape[1], q_ref.shape[1]
    spans = q_ref.shape[0] // SPAN_LEN
    early = k_ref.shape[0] // spans
    late = late_k_ref.shape[0] // spans
    group, groups = pl.program_id(0), width // cols
    lane = lax.broadcasted_iota(jnp.int32, (SPAN_LEN, 128), 1)
    low = lane < HEAD_DIM

    @pl.when(group == 0)
    def _():
        x_ref[...] = rows_of(x_refs, spans)
        total_ref[...] = jnp.zeros_like(total_ref)

    core = where_ref[1]
    last_ref[core] = own_ref[...]
    last_ref[1 - core] = other_ref[...]

    def weight(which):
        return w_ref[:, :, 0, :, which * cols : (which + 1) * cols].reshape(width, cols)

    for target, which in ((late_k_ref, 0), (late_v_ref, 1)):
        target[...] = jnp.dot(x_ref[...], weight(which), preferred_element_type=f32).astype(bf16)
    context_rows = []
    for i in range(spans):
        pieces = []
        first, second = slice(i * early, (i + 1) * early), slice(i * late, (i + 1) * late)
        for pair in range(cols // 128):
            here = slice(pair * 128, pair * 128 + 128)
            qp = q_ref[i * SPAN_LEN : (i + 1) * SPAN_LEN, here]
            zero = jnp.zeros_like(qp)
            two = jnp.concatenate([jnp.where(low, qp, zero), jnp.where(low, zero, qp)], axis=0)
            kp = jnp.concatenate([k_ref[first, here], late_k_ref[second, here]], axis=0)
            vp = jnp.concatenate([v_ref[first, here], late_v_ref[second, here]], axis=0)
            scores = lax.dot_general(
                two, kp, (((1,), (1,)), ((), ())), preferred_element_type=f32
            ) * (HEAD_DIM ** -0.5)
            top = jnp.max(scores, axis=1, keepdims=True)
            raised = jnp.exp(scores - top)
            weights = raised * (1.0 / jnp.sum(raised, axis=1, keepdims=True))
            mixed = jnp.dot(weights.astype(bf16), vp, preferred_element_type=f32)
            pieces.append(jnp.where(low, mixed[:SPAN_LEN], mixed[SPAN_LEN:]).astype(bf16))
        context_rows.append(jnp.concatenate(pieces, axis=1))
    context = jnp.concatenate(context_rows, axis=0)
    total_ref[...] += lax.dot_general(
        context,
        last_ref[:, :, 0].reshape(width, cols),
        (((1,), (1,)), ((), ())),
        preferred_element_type=f32,
    )

    @pl.when(group == groups - 1)
    def _():
        for g in range(groups):
            out_ref[g] = total_ref[:, g * cols : (g + 1) * cols].astype(bf16)


def settings():
    return pltpu.CompilerParams(
        dimension_semantics=("arbitrary",), vmem_limit_bytes=VMEM_BYTES
    )


def prepare(where, chunks, states, weights, other):
    held, width = chunks[0].shape
    groups = weights.shape[1]
    cols = width // groups
    rows = states.shape[0] // groups
    last = states.shape[0] // SPAN_LEN - 1
    keys = held * len(chunks)
    bf16 = jnp.bfloat16

    def after(g, h):
        return jnp.minimum((h[0] + 1) * (rows // SPAN_LEN), last), 0

    def columns(count):
        return pl.BlockSpec((count, cols), lambda g, h: (0, g))

    group = (weights.shape[0], 1, weights.shape[2])
    return pl.pallas_call(
        prepare_kernel,
        out_shape=(
            jax.ShapeDtypeStruct((rows, width), bf16),
            jax.ShapeDtypeStruct((keys, width), bf16),
            jax.ShapeDtypeStruct((keys, width), bf16),
            jax.ShapeDtypeStruct((2, *weights.shape[:3], 2 * cols), bf16),
        ),
        grid_spec=pltpu.PrefetchScalarGridSpec(
            num_scalar_prefetch=1,
            grid=(groups,),
            in_specs=[pl.BlockSpec((held, width), lambda g, h: (0, 0)) for _ in chunks]
            + [
                pl.BlockSpec((rows, width), lambda g, h: (h[0], 0)),
                pl.BlockSpec((SPAN_LEN, width), after),
                pl.BlockSpec((*group, 3 * cols), lambda g, h: (0, g, 0, 0)),
                pl.BlockSpec((*group, 3 * cols), lambda g, h: (0, g, 0, 0)),
            ],
            out_specs=(
                columns(rows),
                columns(keys),
                columns(keys),
                pl.BlockSpec((2, *group, 2 * cols), lambda g, h: (0, 0, g, 0, 0)),
            ),
            scratch_shapes=[
                pltpu.VMEM((keys, width), bf16),
                pltpu.VMEM((rows, width), bf16),
                pltpu.VMEM((2, *group, cols), bf16),
            ],
        ),
        compiler_params=settings(),
        cost_estimate=pl.CostEstimate(
            flops=2 * width * width * (2 * keys + rows),
            bytes_accessed=2 * (keys * width + 4 * weights.size),
            transcendentals=0,
        ),
        name="prepare",
    )(where, *chunks, states, states, weights, other)


def attend(part, where, chunks, queries, keys, values, weights, finals, other):
    held, width = chunks[0].shape
    here = queries.shape[0] // SPAN_LEN // PARTS
    some = held
    rows = here * SPAN_LEN
    early = keys.shape[0] // PARTS
    late = some * len(chunks)
    groups = weights.shape[2]
    cols = width // groups

    def columns(count):
        return pl.BlockSpec((count, cols), lambda g, h: (part, g))

    group = (finals.shape[0], 1, *finals.shape[2:])
    return pl.pallas_call(
        attend_kernel,
        out_shape=jax.ShapeDtypeStruct((groups, rows, cols), jnp.bfloat16),
        grid_spec=pltpu.PrefetchScalarGridSpec(
            num_scalar_prefetch=1,
            grid=(groups,),
            in_specs=[pl.BlockSpec((some, width), lambda g, h: (0, 0)) for _ in chunks]
            + [
                columns(rows),
                columns(early),
                columns(early),
                pl.BlockSpec(
                    weights.shape[:2] + (1,) + weights.shape[3:], lambda g, h: (0, 0, g, 0, 0)
                ),
                pl.BlockSpec(group, lambda g, h: (0, g, 0, 0)),
                pl.BlockSpec(group, lambda g, h: (0, g, 0, 0)),
            ],
            out_specs=pl.BlockSpec((groups, rows, cols), lambda g, h: (0, 0, 0)),
            scratch_shapes=[
                pltpu.VMEM((late, width), jnp.bfloat16),
                pltpu.VMEM((late, cols), jnp.bfloat16),
                pltpu.VMEM((late, cols), jnp.bfloat16),
                pltpu.VMEM((rows, width), jnp.float32),
                pltpu.VMEM((2, *group), jnp.bfloat16),
            ],
        ),
        compiler_params=settings(),
        cost_estimate=pl.CostEstimate(
            flops=2 * width * width * (2 * late + 6 * rows),
            bytes_accessed=2 * (late * width + weights.size),
            transcendentals=0,
        ),
    )(where, *chunks, queries, keys, values, weights, finals, other)


def layer(
    decoder_states, encodings, neighbor_table, query_weight, key_weight, value_weight, out_weight
):
    groups = lax.axis_size("head")
    share = lax.axis_index(("core", "y", "x"))
    head = lax.axis_index("head")
    width = decoder_states.shape[1]

    depth = width // lax.axis_size(("core", "y", "x"))
    part = jnp.concatenate(
        [
            lax.dynamic_slice_in_dim(w, share * depth, depth, 0)
            for w in (key_weight, value_weight, query_weight)
        ]
        + [lax.dynamic_slice_in_dim(out_weight, share * depth, depth, 1).T],
        axis=1,
    )
    passed = [part]
    for step in range(1, groups):
        passed.append(lax.ppermute(part, "head", [(i, (i + step) % groups) for i in range(groups)]))
    order = (head - jnp.arange(groups, dtype=jnp.int32)) % groups
    stacked = jnp.stack(passed)[order]
    shard_ids = neighbor_table[:, :, 0].reshape(-1)
    slot_ids = neighbor_table[:, :, 1].reshape(-1)
    entries = shard_ids.shape[0]
    numbering = jnp.arange(entries, dtype=jnp.int32)
    placed = shard_ids[None, :] == numbering[:, None]
    request = jnp.sum(jnp.where(placed, slot_ids[None, :], 0), axis=1)
    wanted = lax.all_to_all(request, SPAN, split_axis=0, concat_axis=0, tiled=True)
    most = width - width // groups
    weights = lax.all_gather(stacked[:, :, :most], ("y", "x"), axis=0, tiled=True)
    finals = lax.all_gather(stacked[:, :, most:], ("y", "x"), axis=0, tiled=True)
    piece = encodings.shape[1] // CHUNKS
    pieces = encodings.reshape(-1, piece, width)
    sources = shard_ids.reshape(groups, -1)
    flat = ("y", "x", "core")
    z = lax.axis_index("z")
    depth_y, depth_x, depth_z, cores = (lax.axis_size(axis) for axis in SPAN)
    by_plane = wanted.reshape(depth_y, depth_x, depth_z, cores).transpose(2, 0, 1, 3)
    by_plane = by_plane.reshape(depth_z, -1)
    staying, leaving = by_plane[z], by_plane[1 - z]
    sources = (
        sources // 4 * 2
        + sources % 2
        + jnp.where(sources // 2 % 2 == z, 0, by_plane.shape[1])
    )
    crossings = (
        [(p * groups + h, (1 - p) * groups + h) for p in (0, 1) for h in range(groups)],
        [
            (p * groups + h, (1 - p) * groups + (h + (1 if p else -1)) % groups)
            for p in (0, 1)
            for h in range(groups)
        ],
    )

    def exchange(block):
        return lax.all_to_all(block, flat, split_axis=0, concat_axis=0, tiled=True)

    owned = []
    for c in range(CHUNKS):
        crossed = lax.ppermute(
            pieces[CHUNKS * leaving + c], ("z", "head"), crossings[c % 2]
        )
        same = exchange(pieces[CHUNKS * staying + c])
        other = exchange(crossed)
        arrived = jnp.concatenate([same, other], axis=0)
        whole = c < CHUNKS - 1
        for p in range(1 if whole else PARTS):
            taken = sources if whole else jnp.split(sources, PARTS, axis=1)[p]
            blocks = []
            for step in range(groups):
                block = arrived[taken[(head + step) % groups]]
                if step:
                    block = lax.ppermute(
                        block, "head", [(i, (i + step) % groups) for i in range(groups)]
                    )
                blocks.append(block.reshape(-1, width))
            owned.append(blocks)
    weights = weights.reshape(-1, groups, depth, most)
    finals = finals.reshape(-1, groups, depth, width - most)
    other = lax.ppermute(weights, "core", [(0, 1), (1, 0)])
    other_finals = lax.ppermute(finals, "core", [(0, 1), (1, 0)])
    where = jnp.stack([head, lax.axis_index("core")])
    queries, keys, values, weights = prepare(
        where, owned[0], decoder_states, weights, other
    )
    returned = []
    for p in range(PARTS):
        result = attend(
            p, where, owned[1 + p], queries, keys, values, weights, finals, other_finals
        )
        returned.append(
            lax.all_to_all(result, "head", split_axis=0, concat_axis=0, tiled=True)
        )
    columns = jnp.concatenate(returned, axis=1)
    columns = columns.reshape(decoder_states.shape[0], width // groups)
    offset = SPAN_LEN - 1
    return jnp.concatenate(
        [jnp.zeros((offset, columns.shape[1]), columns.dtype), columns[: columns.shape[0] - offset]],
        axis=0,
    )


def solution(mesh):
    fine = jax.sharding.Mesh(mesh.devices.reshape(4, 4, 2, 2, 4), SPAN + ("head",))
    return jax.shard_map(
        layer,
        mesh=fine,
        in_specs=(
            P(SPAN, None),
            P(SPAN, "head", None),
            P(SPAN, None, None),
            P(None, "head"),
            P(None, "head"),
            P(None, "head"),
            P("head", None),
        ),
        out_specs=P(SPAN, "head"),
        check_vma=False,
    )
```

```python
import jax
import jax.numpy as jnp
from jax import lax
from jax.experimental import pallas as pl
from jax.experimental.pallas import tpu as pltpu
from jax.sharding import PartitionSpec as P


HEAD_DIM = 64
SPAN_LEN = 64
SPANS_STEP = 2
CHUNKS = 2
PARTS = 2
VMEM_BYTES = 62 * 1024 * 1024
SPAN = ("y", "x", "z", "core")


def rows_of(x_refs, spans):
    some = x_refs[0].shape[0] // spans
    return jnp.concatenate(
        [x_ref[i * some : (i + 1) * some] for i in range(spans) for x_ref in x_refs], axis=0
    )


def prepare_kernel(where_ref, *refs):
    x_refs = refs[:-10]
    now_ref, next_ref, own_ref, other_ref = refs[-10:-6]
    q_ref, k_ref, v_ref, w_ref, x_ref, states_ref = refs[-6:]
    f32, bf16 = jnp.float32, jnp.bfloat16
    width, cols = x_ref.shape[1], q_ref.shape[1]
    spans = q_ref.shape[0] // SPAN_LEN
    rows = SPANS_STEP * SPAN_LEN

    @pl.when(pl.program_id(0) == 0)
    def _():
        x_ref[...] = rows_of(x_refs, spans)
        row = lax.broadcasted_iota(jnp.int32, (rows, rows + SPAN_LEN), 0)
        col = lax.broadcasted_iota(jnp.int32, (rows, rows + SPAN_LEN), 1)
        shift = jnp.where(col == row + SPAN_LEN - 1, 1.0, 0.0).astype(bf16)
        for first in range(0, spans * SPAN_LEN, rows):
            if first + rows < spans * SPAN_LEN:
                both = now_ref[first : first + rows + SPAN_LEN]
            else:
                both = jnp.concatenate([now_ref[first:], next_ref[...]], axis=0)
            states_ref[first : first + rows] = jnp.dot(
                shift, both, preferred_element_type=f32
            ).astype(bf16)

    core = where_ref[1]
    w_ref[core] = own_ref[...]
    w_ref[1 - core] = other_ref[...]
    for source, target, which in ((x_ref, k_ref, 0), (x_ref, v_ref, 1), (states_ref, q_ref, 2)):
        weight = w_ref[:, :, 0, :, which * cols : (which + 1) * cols].reshape(width, cols)
        target[...] = jnp.dot(source[...], weight, preferred_element_type=f32).astype(bf16)


def attend_kernel(*refs):
    x_refs = refs[:-9]
    q_ref, k_ref, v_ref, w_ref, out_ref, x_ref, late_k_ref, late_v_ref, total_ref = refs[-9:]
    f32, bf16 = jnp.float32, jnp.bfloat16
    width, cols = x_ref.shape[1], q_ref.shape[1]
    spans = q_ref.shape[0] // SPAN_LEN
    early = k_ref.shape[0] // spans
    late = late_k_ref.shape[0] // spans
    group, groups = pl.program_id(0), width // cols
    lane = lax.broadcasted_iota(jnp.int32, (SPAN_LEN, 128), 1)
    low = lane < HEAD_DIM

    @pl.when(group == 0)
    def _():
        x_ref[...] = rows_of(x_refs, spans)
        total_ref[...] = jnp.zeros_like(total_ref)

    def weight(which):
        return w_ref[:, :, 0, :, which * cols : (which + 1) * cols].reshape(width, cols)

    for target, which in ((late_k_ref, 0), (late_v_ref, 1)):
        target[...] = jnp.dot(x_ref[...], weight(which), preferred_element_type=f32).astype(bf16)
    context_rows = []
    for i in range(spans):
        pieces = []
        first, second = slice(i * early, (i + 1) * early), slice(i * late, (i + 1) * late)
        for pair in range(cols // 128):
            here = slice(pair * 128, pair * 128 + 128)
            qp = q_ref[i * SPAN_LEN : (i + 1) * SPAN_LEN, here]
            zero = jnp.zeros_like(qp)
            two = jnp.concatenate([jnp.where(low, qp, zero), jnp.where(low, zero, qp)], axis=0)
            kp = jnp.concatenate([k_ref[first, here], late_k_ref[second, here]], axis=0)
            vp = jnp.concatenate([v_ref[first, here], late_v_ref[second, here]], axis=0)
            scores = lax.dot_general(
                two, kp, (((1,), (1,)), ((), ())), preferred_element_type=f32
            ) * (HEAD_DIM ** -0.5)
            top = jnp.max(scores, axis=1, keepdims=True)
            raised = jnp.exp(scores - top)
            weights = raised * (1.0 / jnp.sum(raised, axis=1, keepdims=True))
            mixed = jnp.dot(weights.astype(bf16), vp, preferred_element_type=f32)
            pieces.append(jnp.where(low, mixed[:SPAN_LEN], mixed[SPAN_LEN:]).astype(bf16))
        context_rows.append(jnp.concatenate(pieces, axis=1))
    context = jnp.concatenate(context_rows, axis=0)
    total_ref[...] += lax.dot_general(
        context, weight(3), (((1,), (1,)), ((), ())), preferred_element_type=f32
    )

    @pl.when(group == groups - 1)
    def _():
        for g in range(groups):
            out_ref[g] = total_ref[:, g * cols : (g + 1) * cols].astype(bf16)


def settings():
    return pltpu.CompilerParams(
        dimension_semantics=("arbitrary",), vmem_limit_bytes=VMEM_BYTES
    )


def prepare(where, chunks, states, weights, other):
    held, width = chunks[0].shape
    groups = weights.shape[1]
    cols = width // groups
    rows = states.shape[0] // groups
    last = states.shape[0] // SPAN_LEN - 1
    keys = held * len(chunks)
    bf16 = jnp.bfloat16

    def after(g, h):
        return jnp.minimum((h[0] + 1) * (rows // SPAN_LEN), last), 0

    def columns(count):
        return pl.BlockSpec((count, cols), lambda g, h: (0, g))

    group = (weights.shape[0], 1) + weights.shape[2:]
    return pl.pallas_call(
        prepare_kernel,
        out_shape=(
            jax.ShapeDtypeStruct((rows, width), bf16),
            jax.ShapeDtypeStruct((keys, width), bf16),
            jax.ShapeDtypeStruct((keys, width), bf16),
            jax.ShapeDtypeStruct((2, *weights.shape), bf16),
        ),
        grid_spec=pltpu.PrefetchScalarGridSpec(
            num_scalar_prefetch=1,
            grid=(groups,),
            in_specs=[pl.BlockSpec((held, width), lambda g, h: (0, 0)) for _ in chunks]
            + [
                pl.BlockSpec((rows, width), lambda g, h: (h[0], 0)),
                pl.BlockSpec((SPAN_LEN, width), after),
                pl.BlockSpec(group, lambda g, h: (0, g, 0, 0)),
                pl.BlockSpec(group, lambda g, h: (0, g, 0, 0)),
            ],
            out_specs=(
                columns(rows),
                columns(keys),
                columns(keys),
                pl.BlockSpec((2, *group), lambda g, h: (0, 0, g, 0, 0)),
            ),
            scratch_shapes=[
                pltpu.VMEM((keys, width), bf16),
                pltpu.VMEM((rows, width), bf16),
            ],
        ),
        compiler_params=settings(),
        cost_estimate=pl.CostEstimate(
            flops=2 * width * width * (2 * keys + rows),
            bytes_accessed=2 * (keys * width + 4 * weights.size),
            transcendentals=0,
        ),
        name="prepare",
    )(where, *chunks, states, states, weights, other)


def attend(part, chunks, queries, keys, values, weights):
    held, width = chunks[0].shape
    here = queries.shape[0] // SPAN_LEN // PARTS
    some = held
    rows = here * SPAN_LEN
    early = keys.shape[0] // PARTS
    late = some * len(chunks)
    groups = weights.shape[2]
    cols = width // groups

    def columns(count):
        return pl.BlockSpec((count, cols), lambda g: (part, g))

    return pl.pallas_call(
        attend_kernel,
        out_shape=jax.ShapeDtypeStruct((groups, rows, cols), jnp.bfloat16),
        grid=(groups,),
        in_specs=[pl.BlockSpec((some, width), lambda g: (0, 0)) for _ in chunks]
        + [
            columns(rows),
            columns(early),
            columns(early),
            pl.BlockSpec(weights.shape[:2] + (1,) + weights.shape[3:], lambda g: (0, 0, g, 0, 0)),
        ],
        out_specs=pl.BlockSpec((groups, rows, cols), lambda g: (0, 0, 0)),
        scratch_shapes=[
            pltpu.VMEM((late, width), jnp.bfloat16),
            pltpu.VMEM((late, cols), jnp.bfloat16),
            pltpu.VMEM((late, cols), jnp.bfloat16),
            pltpu.VMEM((rows, width), jnp.float32),
        ],
        compiler_params=settings(),
        cost_estimate=pl.CostEstimate(
            flops=2 * width * width * (2 * late + 6 * rows),
            bytes_accessed=2 * (late * width + weights.size),
            transcendentals=0,
        ),
    )(*chunks, queries, keys, values, weights)


def layer(
    decoder_states, encodings, neighbor_table, query_weight, key_weight, value_weight, out_weight
):
    groups = lax.axis_size("head")
    share = lax.axis_index(("core", "y", "x"))
    head = lax.axis_index("head")
    width = decoder_states.shape[1]

    depth = width // lax.axis_size(("core", "y", "x"))
    part = jnp.concatenate(
        [
            lax.dynamic_slice_in_dim(w, share * depth, depth, 0)
            for w in (key_weight, value_weight, query_weight)
        ]
        + [lax.dynamic_slice_in_dim(out_weight, share * depth, depth, 1).T],
        axis=1,
    )
    passed = [part]
    for step in range(1, groups):
        passed.append(lax.ppermute(part, "head", [(i, (i + step) % groups) for i in range(groups)]))
    order = (head - jnp.arange(groups, dtype=jnp.int32)) % groups
    stacked = jnp.stack(passed)[order]
    shard_ids = neighbor_table[:, :, 0].reshape(-1)
    slot_ids = neighbor_table[:, :, 1].reshape(-1)
    entries = shard_ids.shape[0]
    numbering = jnp.arange(entries, dtype=jnp.int32)
    placed = shard_ids[None, :] == numbering[:, None]
    request = jnp.sum(jnp.where(placed, slot_ids[None, :], 0), axis=1)
    wanted = lax.all_to_all(request, SPAN, split_axis=0, concat_axis=0, tiled=True)
    weights = lax.all_gather(stacked, "x", axis=0, tiled=True)
    weights = lax.all_gather(weights, "y", axis=0, tiled=True)
    piece = encodings.shape[1] // CHUNKS
    pieces = encodings.reshape(-1, piece, width)
    sources = shard_ids.reshape(groups, -1)
    flat = ("y", "x", "core")
    z = lax.axis_index("z")
    depth_y, depth_x, depth_z, cores = (lax.axis_size(axis) for axis in SPAN)
    by_plane = wanted.reshape(depth_y, depth_x, depth_z, cores).transpose(2, 0, 1, 3)
    by_plane = by_plane.reshape(depth_z, -1)
    staying, leaving = by_plane[z], by_plane[1 - z]
    sources = (
        sources // 4 * 2
        + sources % 2
        + jnp.where(sources // 2 % 2 == z, 0, by_plane.shape[1])
    )
    crossings = (
        [(p * groups + h, (1 - p) * groups + h) for p in (0, 1) for h in range(groups)],
        [
            (p * groups + h, (1 - p) * groups + (h + (1 if p else -1)) % groups)
            for p in (0, 1)
            for h in range(groups)
        ],
    )

    def exchange(block):
        return lax.all_to_all(block, flat, split_axis=0, concat_axis=0, tiled=True)

    owned = []
    for c in range(CHUNKS):
        crossed = lax.ppermute(
            pieces[CHUNKS * leaving + c], ("z", "head"), crossings[c % 2]
        )
        same = exchange(pieces[CHUNKS * staying + c])
        other = exchange(crossed)
        arrived = jnp.concatenate([same, other], axis=0)
        whole = c < CHUNKS - 1
        for p in range(1 if whole else PARTS):
            taken = sources if whole else jnp.split(sources, PARTS, axis=1)[p]
            blocks = []
            for step in range(groups):
                block = arrived[taken[(head + step) % groups]]
                if step:
                    block = lax.ppermute(
                        block, "head", [(i, (i + step) % groups) for i in range(groups)]
                    )
                blocks.append(block.reshape(-1, width))
            owned.append(blocks)
    weights = weights.reshape(-1, groups, depth, width)
    other = lax.ppermute(weights, "core", [(0, 1), (1, 0)])
    where = jnp.stack([head, lax.axis_index("core")])
    queries, keys, values, weights = prepare(
        where, owned[0], decoder_states, weights, other
    )
    returned = []
    for p in range(PARTS):
        result = attend(p, owned[1 + p], queries, keys, values, weights)
        returned.append(
            lax.all_to_all(result, "head", split_axis=0, concat_axis=0, tiled=True)
        )
    columns = jnp.concatenate(returned, axis=1)
    columns = columns.reshape(decoder_states.shape[0], width // groups)
    offset = SPAN_LEN - 1
    return jnp.concatenate(
        [jnp.zeros((offset, columns.shape[1]), columns.dtype), columns[: columns.shape[0] - offset]],
        axis=0,
    )


def solution(mesh):
    fine = jax.sharding.Mesh(mesh.devices.reshape(4, 4, 2, 2, 4), SPAN + ("head",))
    return jax.shard_map(
        layer,
        mesh=fine,
        in_specs=(
            P(SPAN, None),
            P(SPAN, "head", None),
            P(SPAN, None, None),
            P(None, "head"),
            P(None, "head"),
            P(None, "head"),
            P("head", None),
        ),
        out_specs=P(SPAN, "head"),
        check_vma=False,
    )
```
